32 devices in a mesh: col: 8 (over y, x, core), row: 4 (over z).
Axes of the slice: x: 2, y: 2, z: 4, core: 2. Of those that a mesh axis runs over, the one named last changes fastest.
Arguments:
- visibilities: bfloat16 [2, 8192, 4096], P(None, 'col', 'row'), may hold values from -6 to 6
- col_offsets: int32 [8], P('col'), may hold values from 0 to 15360
- row_offsets: int32 [4], replicated, may hold values from 0 to 15360
- facet_offsets: int32 [8, 2], replicated, may hold values from 0 to 16383
- facet_order: int32 [8], replicated, may hold values from 0 to 7, each once
- vis_counts: int32 [8, 4], P('col', 'row'), may hold values from 512 to 1024
Outputs:
- facet_images: float32 [8, 2, 64, 4096], P('col', None, None, 'row')
- peak: float32 [8], P('col')
The draws below stay inside these ranges and needn't reach their ends.
Inputs may be any that keep to these rules, and one draw needn't show every extreme that they name: `facet_order`: each slot names a different facet.
All inputs are finite; a program needn't handle non-finite values.
Results may differ from the reference program's by a relative error of at most 0.0078.
Values may be sent and summed in bfloat16 or wider, within the bound.
A program may use at most 128 MiB of HBM per device.

```python
import math
import jax
import jax.numpy as jnp
from jax import lax

M = 1024
FS = 4096
NG = 16384
FR = 64
NFACET = 8
N_COL = 8
N_ROW = 4


def with_ends(entries, rng, least, largest):
    extent = entries.shape
    place = [jax.random.randint(jax.random.fold_in(rng, axis), (), 0, extent[axis]) for axis in range(len(extent))]
    entries = entries.at[tuple(place)].set(least)
    longest = extent.index(max(extent))
    place[longest] = (place[longest] + 1) % extent[longest]
    return entries.at[tuple(place)].set(largest)


def steps_of(key, dims, pieces, low, high):
    gain = 1.0
    for dim, blocks in pieces:
        steps = jax.random.uniform(jax.random.fold_in(jax.random.fold_in(key, 6), dim), (blocks,), jnp.float32, low / len(pieces), high / len(pieces))
        gain = gain * jnp.repeat(jnp.exp(steps), dims[dim] // blocks).reshape((-1,) + (1,) * (len(dims) - 1 - dim))
    return gain


def noise(own_key, shape, width, reach, cuts=(), kind=jnp.bfloat16):
    result = jax.random.normal(own_key, shape, jnp.float32) * width
    if len(cuts) > 0:
        result = steps_of(own_key, shape, cuts, -0.22, 0.18) * result
    return jnp.clip(result, min=-reach, max=reach).astype(kind)


def setup_inputs(seed: int = 0) -> dict:
    arg_keys = jax.random.split(jax.random.key(seed), 7)
    return {
        "visibilities": noise(arg_keys[0], (2, N_COL * M, N_ROW * M), 1.0, 6.0, ((1, 8), (2, 4))),
        "col_offsets": with_ends(jax.random.randint(arg_keys[1], (N_COL,), 0, NG - M + 1), jax.random.fold_in(arg_keys[1], 1), 0, NG - M).astype(jnp.int32),
        "row_offsets": with_ends(jax.random.randint(arg_keys[2], (N_ROW,), 0, NG - M + 1), jax.random.fold_in(arg_keys[2], 1), 0, NG - M).astype(jnp.int32),
        "facet_offsets": with_ends(jax.random.randint(arg_keys[3], (NFACET, 2), 0, NG), jax.random.fold_in(arg_keys[3], 1), 0, NG - 1).astype(jnp.int32),
        "facet_order": jax.random.permutation(arg_keys[4], NFACET).astype(jnp.int32),
        "vis_counts": with_ends(jax.random.randint(arg_keys[5], (N_COL, N_ROW), M // 2, M + 1), jax.random.fold_in(arg_keys[5], 1), M // 2, M).astype(jnp.int32),
    }


TWO_PI = 2.0 * math.pi
BEAM_SLOPE = 0.66

def phase_table(first_ids, second_ids, factor):
    product = first_ids[:, None] * second_ids[None, :] % NG
    angles = product.astype(jnp.float32) * (TWO_PI / NG)
    return ((jnp.cos(angles) * factor).astype(jnp.bfloat16), (jnp.sin(angles) * factor).astype(jnp.bfloat16))

def complex_product(left_real, left_imag, right_real, right_imag):
    left_rows = jnp.concatenate([left_real, left_imag], axis=0)
    right_cols = jnp.concatenate([right_real, right_imag], axis=1)
    product = jnp.dot(left_rows, right_cols, preferred_element_type=jnp.float32)
    product = product.reshape(2, left_real.shape[0], 2, right_real.shape[1])
    real_part = product[0, :, 0] - product[1, :, 1]
    imag_part = product[0, :, 1] + product[1, :, 0]
    return (real_part, imag_part)

def reference(visibilities, col_offsets, row_offsets, facet_offsets, facet_order, vis_counts):
    slot_pick = (facet_order[:, None] == jnp.arange(NFACET, dtype=jnp.int32)[None, :]).astype(jnp.int32)
    slot_offsets = lax.optimization_barrier(jnp.sum(slot_pick[:, :, None] * facet_offsets[None, :, :], axis=1))
    row_ids = jnp.arange(M, dtype=jnp.int32)
    pixel_rows = jnp.arange(FR, dtype=jnp.int32) + (FS // 2 - FR // 2)
    pixel_cols = jnp.arange(FS, dtype=jnp.int32)
    grid_u = (col_offsets[:, None] + row_ids[None, :]).reshape(N_COL * M)
    first_scale = 1.0 / math.sqrt(M * N_COL)
    second_scale = 0.5 / math.sqrt(M * N_ROW)

    def add_row(running, row_index):
        column_strip = lax.dynamic_slice_in_dim(visibilities, (row_index * M).astype(jnp.int32), M, 2)
        counts_here = lax.dynamic_index_in_dim(vis_counts, row_index, 1, keepdims=False)
        live_rows = (row_ids[None, :] < counts_here[:, None]).reshape(N_COL * M)
        column_strip = jnp.where(live_rows[None, :, None], column_strip, jnp.zeros_like(column_strip))
        grid_v = lax.dynamic_index_in_dim(row_offsets, row_index, 0, keepdims=False) + row_ids

        def one_slot(slot_index):
            offsets = lax.dynamic_index_in_dim(slot_offsets, slot_index, 0, keepdims=False)
            image_rows = (offsets[0] + pixel_rows) % NG
            table_real, table_imag = phase_table(image_rows, grid_u, first_scale)
            part_real, part_imag = complex_product(table_real, table_imag, column_strip[0], column_strip[1])
            columns = jnp.stack([part_real, part_imag], axis=0).astype(jnp.bfloat16)
            image_cols = (offsets[1] + pixel_cols) % NG
            second_real, second_imag = phase_table(grid_v, image_cols, second_scale)
            out_real, out_imag = complex_product(columns[0], columns[1], second_real, second_imag)
            return jnp.stack([out_real, out_imag], axis=0)
        return (running + lax.map(one_slot, jnp.arange(NFACET, dtype=jnp.int32)), None)
    initial = jnp.zeros((NFACET, 2, FR, FS), jnp.float32)
    facet_sum, ignored = lax.scan(add_row, initial, jnp.arange(N_ROW, dtype=jnp.int32))
    beam = 1.0 - BEAM_SLOPE * (pixel_cols.astype(jnp.float32) + 0.5) / FS
    facet_images = facet_sum / beam[None, None, None, :]
    magnitude = jnp.sqrt(facet_images[:, 0] * facet_images[:, 0] + facet_images[:, 1] * facet_images[:, 1])
    peak = lax.optimization_barrier(jnp.max(magnitude, axis=(1, 2)))
    return (facet_images, peak)
```

```python
import functools
import math

import jax
import jax.numpy as jnp
from jax import lax
from jax.experimental import pallas as pl
from jax.experimental.pallas import tpu as pltpu
from jax.sharding import PartitionSpec as P

FS = 4096
NG = 16384
FR = 64
TWO_PI = 2.0 * math.pi
BEAM_SLOPE = 0.66
FINE = 32
GROUPS = 4
HALVES = 2
CHUNKS = GROUPS * HALVES
MESH = pl.DeviceIdType.MESH
F32 = jnp.float32
BF16 = jnp.bfloat16


def cis(product):
    shift = (NG // 4).bit_length() - 1
    turn = product & (NG - 1)
    quadrant = (turn + NG // 8) >> shift
    rest = turn - (quadrant << shift)
    angle = rest.astype(F32) * (TWO_PI / NG)
    z = angle * angle
    sine = angle * (1.0 + z * (-1.0 / 6 + z * (1.0 / 120 + z * (-1.0 / 5040 + z * (1.0 / 362880)))))
    cosine = 1.0 + z * (-0.5 + z * (1.0 / 24 + z * (-1.0 / 720 + z * (1.0 / 40320))))
    odd = (quadrant & 1) == 1
    real = jnp.where(odd, sine, cosine)
    imag = jnp.where(odd, cosine, sine)
    real = jnp.where(((quadrant + 1) & 2) != 0, -real, real)
    imag = jnp.where((quadrant & 2) != 0, -imag, imag)
    return real, imag


def iota(shape, dim):
    return lax.broadcasted_iota(jnp.int32, shape, dim)


def kernel(
    cols, rows,
    vis_hbm, *refs,
):
    small, (image, peak), scratch = refs[:5], refs[5:7], refs[7:]
    (
    col_off, row_off, facet_off, facet_order, counts, small_sem,
    vis, head, fine, table, mine, pair_out, pair_in, sums, others, gathered,
    coarse2, fine2, table2, phases, relay_out, relay_in, best, peaks,
    vis_sem, pair_send, pair_recv, col_send, col_recv, row_send, row_recv,
    relay_send, relay_recv, peak_send, peak_recv,
    ) = scratch
    copies = [
        pltpu.make_async_copy(source, target, small_sem.at[n])
        for n, (source, target) in enumerate(zip(small, scratch[:5]))
    ]
    for copy in copies:
        copy.start()
    m = vis.shape[1]
    width = m // HALVES
    group = FR // GROUPS
    chips = cols // 2
    block_cols = FS // rows
    me_col = lax.axis_index("col")
    me_row = lax.axis_index("row")
    core = lax.rem(me_col, 2)
    chip = me_col // 2
    partner = chip * 2 + 1 - core
    inner = (me_row >= 1) & (me_row <= rows - 2)
    outer = (me_row == 0) | (me_row == rows - 1)
    helps = (me_row == 1) | (me_row == rows - 2)
    end_row = jnp.where(me_row <= 1, 0, rows - 1)
    helper = jnp.where(me_row <= 1, 1, rows - 2)

    def peer_chip(d):
        return lax.rem(chip + d, chips) * 2 + core

    def peer_row(d):
        return lax.rem(me_row + d, rows)

    barrier = pltpu.get_barrier_semaphore()
    pl.semaphore_signal(barrier, inc=1, device_id=(partner, me_row), device_id_type=MESH)
    for d in range(1, chips):
        pl.semaphore_signal(barrier, inc=1, device_id=(peer_chip(d), me_row), device_id_type=MESH)
    for d in range(1, rows):
        pl.semaphore_signal(barrier, inc=1, device_id=(me_col, peer_row(d)), device_id_type=MESH)

    def vis_copy(h, ri):
        part = pl.ds(h * width, width)
        return pltpu.make_async_copy(vis_hbm.at[ri, :, part], vis.at[ri, :, part], vis_sem.at[h, ri])

    for h in range(HALVES):
        for ri in range(2):
            vis_copy(h, ri).start()

    with jax.named_scope("small"):
        for copy in copies:
            copy.wait()

    u = iota((cols, m), 1)
    slot = iota((cols, m), 0)
    start = jnp.zeros((cols, m), jnp.int32)
    for half in range(2):
        for c in range(chips):
            facet = facet_order[c * 2 + (core if half == 0 else 1 - core)]
            first = (facet_off[0, facet] + (FS // 2 - FR // 2)) & (NG - 1)
            start = jnp.where(slot == half * chips + c, first, start)
    real, imag = cis(start * (col_off[0] + u))
    scale = jnp.where(u < counts[0, 0], 1.0 / math.sqrt(m * cols), 0.0)
    head[0] = real * scale
    head[1] = imag * scale
    real, imag = cis(iota((FR, m), 0) * (col_off[0] + iota((FR, m), 1)))
    fine[0] = real
    fine[1] = imag
    block = cols * group
    dot = functools.partial(jnp.dot, preferred_element_type=F32)

    def column_table(g):
        for s in range(cols):
            a, b = head[0, pl.ds(s, 1), :], head[1, pl.ds(s, 1), :]
            c, d = fine[0, pl.ds(g * group, group), :], fine[1, pl.ds(g * group, group), :]
            imag = a * d + b * c
            table[g, pl.ds(s * group, group), :] = (-imag).astype(BF16)
            table[g, pl.ds(block + s * group, group), :] = (a * c - b * d).astype(BF16)
            table[g, pl.ds(2 * block + s * group, group), :] = imag.astype(BF16)

    def pair_copy(n):
        return pltpu.make_async_remote_copy(
            src_ref=pair_out.at[n], dst_ref=pair_in.at[n],
            send_sem=pair_send.at[n], recv_sem=pair_recv.at[n],
            device_id=(partner, me_row), device_id_type=MESH)

    def col_copy(n, d):
        target = lax.rem(chip + d, chips)
        return pltpu.make_async_remote_copy(
            src_ref=sums.at[n, target], dst_ref=others.at[n, d - 1],
            send_sem=col_send.at[n, d - 1], recv_sem=col_recv.at[n, d - 1],
            device_id=(target * 2 + core, me_row), device_id_type=MESH)

    def row_copy(n, origin, target):
        return pltpu.make_async_remote_copy(
            src_ref=gathered.at[n, origin], dst_ref=gathered.at[n, origin],
            send_sem=row_send.at[n, target], recv_sem=row_recv.at[n, origin],
            device_id=(me_col, target), device_id_type=MESH)

    def relay_copy(g, target):
        return pltpu.make_async_remote_copy(
            src_ref=relay_out.at[g], dst_ref=relay_in.at[g],
            send_sem=relay_send.at[g], recv_sem=relay_recv.at[g],
            device_id=(me_col, target), device_id_type=MESH)

    def peak_copy(origin, target):
        return pltpu.make_async_remote_copy(
            src_ref=peaks.at[origin], dst_ref=peaks.at[origin],
            send_sem=peak_send.at[target], recv_sem=peak_recv.at[origin],
            device_id=(me_col, target), device_id_type=MESH)

    def each_inner_row(act):
        for dist in range(rows - 1, 0, -1):
            for step in (dist, -dist):
                target = me_row + step

                @pl.when((target >= 1) & (target <= rows - 2))
                def _():
                    act(target)

    def transform(n):
        g, h = n // HALVES, n % HALVES
        if g == 0:
            vis_copy(h, 0).wait()
            vis_copy(h, 1).wait()
        part = pl.ds(h * width, width)
        both = dot(table[g, pl.ds(block, 2 * block), :], vis[0, :, part])
        both += dot(table[g, pl.ds(0, 2 * block), :], vis[1, :, part])
        both = both.reshape(2, 2, chips, group, width)
        for ri in range(2):
            pair_out[n, :, pl.ds(ri * group, group), :] = both[ri, 1].astype(BF16)
            mine[n, :, pl.ds(ri * group, group), :] = both[ri, 0]

    def pair_sum(n):
        pair_copy(n).wait_recv()
        sums[n] = (mine[n] + pair_in[n].astype(F32)).astype(BF16)
        for d in range(chips - 1, 0, -1):
            col_copy(n, d).start()

    def facet_sum(n):
        total = mine[n, chip] + pair_in[n, chip].astype(F32)
        for d in range(1, chips):
            col_copy(n, d).wait_recv()
            total = total + others[n, d - 1].astype(F32)
        gathered[n, me_row] = total.astype(BF16)
        each_inner_row(lambda target: row_copy(n, me_row, target).start())

    def row_table(at, block_row):
        column0 = (facet_off[1, facet_order[me_col]] + block_row * block_cols) & (NG - 1)
        shape = (m // FINE, block_cols)
        real, imag = cis(iota(shape, 0) * FINE * (column0 + iota(shape, 1)))
        coarse2[0] = real
        coarse2[1] = imag
        shape = (FINE, block_cols)
        real, imag = cis(iota(shape, 0) * (column0 + iota(shape, 1)))
        fine2[0] = real
        fine2[1] = imag

        def fill(h, carry):
            a, b = coarse2[0, pl.ds(h, 1), :], coarse2[1, pl.ds(h, 1), :]
            c, d = fine2[0], fine2[1]
            out = pl.ds(pl.multiple_of(h * FINE, FINE), FINE)
            table2[at, 0, out, :] = (a * c - b * d).astype(BF16)
            table2[at, 1, out, :] = (a * d + b * c).astype(BF16)
            return carry

        lax.fori_loop(0, m // FINE, fill, 0)
        row_ids = iota((rows, block_cols), 0)
        offsets = jnp.zeros((rows, block_cols), jnp.int32)
        for r in range(rows):
            offsets = jnp.where(row_ids == r, row_off[r], offsets)
        lanes = iota((rows, block_cols), 1)
        beam = 1.0 - BEAM_SLOPE * ((block_row * block_cols + lanes).astype(F32) + 0.5) / FS
        gain = (0.5 / math.sqrt(m * rows)) / beam
        real, imag = cis(offsets * ((column0 + lanes) & (NG - 1)))
        phases[at, 0] = real * gain
        phases[at, 1] = imag * gain

    piece = min(512, block_cols)

    def second(g, at):
        strongest = best[...]
        for c0 in range(0, block_cols, piece):
            part = pl.ds(c0, piece)
            sides = []
            for side in range(2):
                product = None
                for h in range(HALVES):
                    left = gathered[g * HALVES + h].reshape(rows * 2 * group, width)
                    term = dot(left, table2[at, side, pl.ds(h * width, width), part])
                    product = term if product is None else product + term
                sides.append(product.reshape(rows, 2, group, piece))
            out_real = jnp.zeros((group, piece), F32)
            out_imag = jnp.zeros((group, piece), F32)
            for r in range(rows):
                real = sides[0][r, 0] - sides[1][r, 1]
                imag = sides[1][r, 0] + sides[0][r, 1]
                a, b = phases[at, 0, pl.ds(r, 1), part], phases[at, 1, pl.ds(r, 1), part]
                out_real = out_real + (real * a - imag * b)
                out_imag = out_imag + (real * b + imag * a)
            if at == 0:
                image[0, 0, pl.ds(g * group, group), part] = out_real
                image[0, 1, pl.ds(g * group, group), part] = out_imag
            else:
                relay_out[g, pl.ds(0, group), part] = out_real.astype(BF16)
                relay_out[g, pl.ds(group, group), part] = out_imag.astype(BF16)
            power = out_real * out_real + out_imag * out_imag
            power = jnp.max(power.reshape(group // 8, 8, piece), axis=0)
            for lane in range(0, piece, 128):
                strongest = jnp.maximum(strongest, power[:, lane : lane + 128])
        best[...] = strongest

    def row_group(g):
        for h in range(HALVES):
            for origin in range(rows):
                @pl.when(me_row != origin)
                def _():
                    row_copy(g * HALVES + h, origin, origin).wait_recv()

        @pl.when(helps)
        def _():
            second(g, 1)
            relay_copy(g, end_row).start()

        second(g, 0)

    best[...] = jnp.zeros(best.shape, F32)
    for n in range(CHUNKS):
        if n % HALVES == 0:
            with jax.named_scope(f"table{n}"):
                column_table(n // HALVES)
        with jax.named_scope(f"tr{n}"):
            transform(n)
        with jax.named_scope(f"send{n}"):
            if n == 0:
                pl.semaphore_wait(barrier, chips + rows - 1)
            pair_copy(n).start()
        if n > 0:
            with jax.named_scope(f"pair{n - 1}"):
                pair_sum(n - 1)
    with jax.named_scope("pairlast"):
        pair_sum(CHUNKS - 1)

    for n in range(CHUNKS):
        with jax.named_scope(f"facet{n}"):
            facet_sum(n)
        if n == 0:
            @pl.when(inner)
            def _():
                with jax.named_scope("rowtab0"):
                    row_table(0, me_row)
        if n == 1:
            @pl.when(helps)
            def _():
                with jax.named_scope("rowtab1"):
                    row_table(1, end_row)
        ready = n - HALVES - 2
        if ready >= 0 and ready % HALVES == 0 and n < CHUNKS - 1:
            @pl.when(inner)
            def _():
                with jax.named_scope(f"group{ready // HALVES}"):
                    row_group(ready // HALVES)
    for g in range((CHUNKS - 2 - HALVES - 2) // HALVES + 1, GROUPS):
        @pl.when(inner)
        def _():
            with jax.named_scope(f"group{g}"):
                row_group(g)

    @pl.when(inner)
    def _():
        peaks[me_row] = jnp.sqrt(best[...])
        for d in range(1, rows):
            peak_copy(me_row, peer_row(d)).start()

    @pl.when(outer)
    def _():
        for g in range(GROUPS):
            with jax.named_scope(f"relay{g}"):
                relay_copy(g, helper).wait_recv()
                for ri in range(2):
                    image[0, ri, pl.ds(g * group, group), :] = relay_in[g, pl.ds(ri * group, group), :].astype(F32)

    with jax.named_scope("sends"):
        for n in range(CHUNKS):
            pair_copy(n).wait_send()
            for d in range(1, chips):
                col_copy(n, d).wait_send()
            each_inner_row(lambda target: row_copy(n, me_row, target).wait_send())

        @pl.when(helps)
        def _():
            for g in range(GROUPS):
                relay_copy(g, end_row).wait_send()

    with jax.named_scope("peakwait"):
        for origin in range(1, rows - 1):
            @pl.when(me_row != origin)
            def _():
                peak_copy(origin, origin).wait_recv()

        @pl.when(inner)
        def _():
            for d in range(1, rows):
                peak_copy(me_row, peer_row(d)).wait_send()

        strongest = peaks[1]
        for r in range(2, rows - 1):
            strongest = jnp.maximum(strongest, peaks[r])
        peak[0] = jnp.max(strongest)


def local(cols, rows, visibilities, col_offsets, row_offsets, facet_offsets, facet_order, vis_counts):
    m = visibilities.shape[1]
    width = m // HALVES
    group = FR // GROUPS
    chips = cols // 2
    block_cols = FS // rows
    dma = pltpu.SemaphoreType.DMA
    smem = pl.BlockSpec(memory_space=pltpu.SMEM)
    anywhere = pl.BlockSpec(memory_space=pl.ANY)
    small = (col_offsets, row_offsets, facet_offsets.T, facet_order, vis_counts)
    return pl.pallas_call(
        functools.partial(kernel, cols, rows),
        out_shape=(
            pltpu.VMEM((1, 2, FR, block_cols), F32),
            jax.ShapeDtypeStruct((1,), F32),
        ),
        in_specs=[anywhere] * 6,
        out_specs=(pl.BlockSpec(memory_space=pltpu.VMEM), smem),
        scratch_shapes=[pltpu.SMEM(x.shape, x.dtype) for x in small] + [
            dma((len(small),)),
            pltpu.VMEM((2, m, m), BF16),
            pltpu.VMEM((2, cols, m), F32),
            pltpu.VMEM((2, FR, m), F32),
            pltpu.VMEM((GROUPS, 3 * cols * group, m), BF16),
            pltpu.VMEM((CHUNKS, chips, 2 * group, width), F32),
            pltpu.VMEM((CHUNKS, chips, 2 * group, width), BF16),
            pltpu.VMEM((CHUNKS, chips, 2 * group, width), BF16),
            pltpu.VMEM((CHUNKS, chips, 2 * group, width), BF16),
            pltpu.VMEM((CHUNKS, chips - 1, 2 * group, width), BF16),
            pltpu.VMEM((CHUNKS, rows, 2 * group, width), BF16),
            pltpu.VMEM((2, m // FINE, block_cols), F32),
            pltpu.VMEM((2, FINE, block_cols), F32),
            pltpu.VMEM((2, 2, m, block_cols), BF16),
            pltpu.VMEM((2, 2, rows, block_cols), F32),
            pltpu.VMEM((GROUPS, 2 * group, block_cols), BF16),
            pltpu.VMEM((GROUPS, 2 * group, block_cols), BF16),
            pltpu.VMEM((8, 128), F32),
            pltpu.VMEM((rows, 8, 128), F32),
            dma((HALVES, 2)),
            dma((CHUNKS,)),
            dma((CHUNKS,)),
            dma((CHUNKS, chips - 1)),
            dma((CHUNKS, chips - 1)),
            dma((CHUNKS, rows)),
            dma((CHUNKS, rows)),
            dma((GROUPS,)),
            dma((GROUPS,)),
            dma((rows,)),
            dma((rows,)),
        ],
        compiler_params=pltpu.CompilerParams(
            collective_id=0, has_side_effects=True, vmem_limit_bytes=60 * 1024 * 1024),
    )(visibilities, *small)


def solution(mesh):
    in_specs = (P(None, "col", "row"), P("col"), P(), P(), P(), P("col", "row"))
    out_specs = (P("col", None, None, "row"), P("col"))
    body = functools.partial(local, mesh.shape["col"], mesh.shape["row"])
    return jax.shard_map(body, mesh=mesh, in_specs=in_specs, out_specs=out_specs, check_vma=False)
```

```python
import functools
import math

import jax
import jax.numpy as jnp
from jax import lax
from jax.experimental import pallas as pl
from jax.experimental.pallas import tpu as pltpu
from jax.sharding import PartitionSpec as P

FS = 4096
NG = 16384
FR = 64
TWO_PI = 2.0 * math.pi
BEAM_SLOPE = 0.66
FINE = 32
GROUPS = 4
ORDER = (
    "T0 T1 R0 P0 T2 P1 T3 P2 T4 P3 T5 P4 T6 P5 F0 T7 P6 F1 T8 P7 T9 P8 F2 P9 B0 F3 B1 B2",
    "F4 B3 R1 B4 F5 B5 B6 B7 F6 E0 F7 S0 F8 F9 E1 S1 E2 S2 E3 S3",
)
MESH = pl.DeviceIdType.MESH
F32 = jnp.float32
BF16 = jnp.bfloat16


def cis(product):
    shift = (NG // 4).bit_length() - 1
    turn = product & (NG - 1)
    quadrant = (turn + NG // 8) >> shift
    rest = turn - (quadrant << shift)
    angle = rest.astype(F32) * (TWO_PI / NG)
    z = angle * angle
    sine = angle * (1.0 + z * (-1.0 / 6 + z * (1.0 / 120 + z * (-1.0 / 5040 + z * (1.0 / 362880)))))
    cosine = 1.0 + z * (-0.5 + z * (1.0 / 24 + z * (-1.0 / 720 + z * (1.0 / 40320))))
    odd = (quadrant & 1) == 1
    real = jnp.where(odd, sine, cosine)
    imag = jnp.where(odd, cosine, sine)
    real = jnp.where(((quadrant + 1) & 2) != 0, -real, real)
    imag = jnp.where((quadrant & 2) != 0, -imag, imag)
    return real, imag


def iota(shape, dim):
    return lax.broadcasted_iota(jnp.int32, shape, dim)


def chunk_plan(m):
    half, quarter = m // 2, m // 4
    plan = []
    for g in range(GROUPS):
        for h in range(2):
            if (g, h) in ((0, 0), (GROUPS - 1, 1)):
                plan += [(g, h * half, quarter), (g, h * half + quarter, quarter)]
            else:
                plan.append((g, h * half, half))
    return plan


def kernel(
    cols, rows, plan,
    vis_hbm, *refs,
):
    small, (image, peak), scratch = refs[:5], refs[5:7], refs[7:]
    (
    col_off, row_off, facet_off, facet_order, counts, small_sem,
    vis, head, fine, table, mine, pair_out, pair_in, sums, others, gathered,
    coarse2, fine2, table2, phases, relay_out, relay_in, best, peaks,
    vis_sem, pair_send, pair_recv, col_send, col_recv, row_send, row_recv,
    relay_send, relay_recv, peak_send, peak_recv,
    ) = scratch
    copies = [
        pltpu.make_async_copy(source, target, small_sem.at[n])
        for n, (source, target) in enumerate(zip(small, scratch[:5]))
    ]
    for copy in copies:
        copy.start()
    m = vis.shape[1]
    group = FR // GROUPS
    chips = cols // 2
    block_cols = FS // rows
    piece = min(512, block_cols)
    chunks = len(plan)
    me_col = lax.axis_index("col")
    me_row = lax.axis_index("row")
    core = lax.rem(me_col, 2)
    chip = me_col // 2
    partner = chip * 2 + 1 - core
    inner = (me_row >= 1) & (me_row <= rows - 2)
    outer = (me_row == 0) | (me_row == rows - 1)
    helps = (me_row == 1) | (me_row == rows - 2)
    end_row = jnp.where(me_row <= 1, 0, rows - 1)

    def peer_chip(d):
        return lax.rem(chip + d, chips) * 2 + core

    def peer_row(d):
        return lax.rem(me_row + d, rows)

    barrier = pltpu.get_barrier_semaphore()
    pl.semaphore_signal(barrier, inc=1, device_id=(partner, me_row), device_id_type=MESH)
    for d in range(1, chips):
        pl.semaphore_signal(barrier, inc=1, device_id=(peer_chip(d), me_row), device_id_type=MESH)
    for d in range(1, rows):
        pl.semaphore_signal(barrier, inc=1, device_id=(me_col, peer_row(d)), device_id_type=MESH)

    strips = [(v0, width) for g, v0, width in plan if g == 0]

    def vis_copy(h):
        part = pl.ds(*strips[h])
        return pltpu.make_async_copy(vis_hbm.at[:, :, part], vis.at[:, :, part], vis_sem.at[h])

    for h in range(len(strips)):
        vis_copy(h).start()

    real, imag = cis(iota((FR, m), 0) * iota((FR, m), 1))
    fine[0] = real
    fine[1] = imag
    best[...] = jnp.zeros(best.shape, F32)

    with jax.named_scope("small"):
        for copy in copies:
            copy.wait()

    u = iota((cols, m), 1)
    slot = iota((cols, m), 0)
    start = jnp.zeros((cols, m), jnp.int32)
    for half in range(2):
        for c in range(chips):
            facet = facet_order[c * 2 + (core if half == 0 else 1 - core)]
            first = (facet_off[0, facet] + (FS // 2 - FR // 2)) & (NG - 1)
            start = jnp.where(slot == half * chips + c, first, start)
    real, imag = cis(start * (col_off[0] + u))
    scale = jnp.where(u < counts[0, 0], 1.0 / math.sqrt(m * cols), 0.0)
    head[0] = real * scale
    head[1] = imag * scale
    turns = cis(iota((FR, 128), 0) * col_off[0])
    block = cols * group
    dot = functools.partial(jnp.dot, preferred_element_type=F32)

    def column_table(g):
        rows_here = slice(g * group, (g + 1) * group)
        a, b = (jnp.concatenate([x[rows_here]] * (m // 128), axis=1) for x in turns)
        c, d = fine[0, rows_here, :], fine[1, rows_here, :]
        c, d = a * c - b * d, a * d + b * c
        for s in range(cols):
            a, b = head[0, pl.ds(s, 1), :], head[1, pl.ds(s, 1), :]
            imag = a * d + b * c
            real = a * c - b * d
            table[g, pl.ds(s * group, group), :] = real.astype(BF16)
            table[g, pl.ds(block + s * group, group), :] = imag.astype(BF16)
            table[g, pl.ds(2 * block + s * group, group), :] = (-real).astype(BF16)

    def pair_copy(n):
        g, v0, width = plan[n]
        part = pl.ds(v0, width)
        return pltpu.make_async_remote_copy(
            src_ref=pair_out.at[g, :, :, part], dst_ref=pair_in.at[g, :, :, part],
            send_sem=pair_send, recv_sem=pair_recv.at[n],
            device_id=(partner, me_row), device_id_type=MESH)

    def col_copy(n, d):
        g, v0, width = plan[n]
        part = pl.ds(v0, width)
        target = lax.rem(chip + d, chips)
        return pltpu.make_async_remote_copy(
            src_ref=sums.at[g, target, :, part], dst_ref=others.at[g, d - 1, :, part],
            send_sem=col_send, recv_sem=col_recv.at[n],
            device_id=(target * 2 + core, me_row), device_id_type=MESH)

    def row_copy(n, target):
        g, v0, width = plan[n]
        part = pl.ds(v0, width)
        return pltpu.make_async_remote_copy(
            src_ref=gathered.at[g, me_row, :, part], dst_ref=gathered.at[g, me_row, :, part],
            send_sem=row_send, recv_sem=row_recv.at[g],
            device_id=(me_col, target), device_id_type=MESH)

    def relay_copy(g, p):
        return pltpu.make_async_remote_copy(
            src_ref=relay_out.at[g, p], dst_ref=relay_in.at[g, p],
            send_sem=relay_send, recv_sem=relay_recv.at[g],
            device_id=(me_col, end_row), device_id_type=MESH)

    def peak_copy(target):
        return pltpu.make_async_remote_copy(
            src_ref=peaks.at[me_row], dst_ref=peaks.at[me_row],
            send_sem=peak_send, recv_sem=peak_recv,
            device_id=(me_col, target), device_id_type=MESH)

    def wait_bytes(ref, sem):
        pltpu.make_async_copy(ref, ref, sem).wait()

    def each_inner_row(act):
        for dist in range(rows - 1, 0, -1):
            for step in (dist, -dist):
                target = me_row + step

                @pl.when((target >= 1) & (target <= rows - 2))
                def _():
                    act(target)

    def transform(n):
        g, v0, width = plan[n]
        part = pl.ds(v0, width)
        if g == 0:
            vis_copy(n).wait()
        both = dot(table[g, pl.ds(0, 2 * block), :], vis[0, :, part])
        both = both - dot(table[g, pl.ds(block, 2 * block), :], vis[1, :, part])
        both = both.reshape(2, 2, chips, group, width)
        for ri in range(2):
            pair_out[g, :, pl.ds(ri * group, group), part] = both[ri, 1].astype(BF16)
            mine[g, :, pl.ds(ri * group, group), part] = both[ri, 0]

    def pair_sum(n):
        pair_copy(n).wait_recv()
        g, v0, width = plan[n]
        part = pl.ds(v0, width)
        sums[g, :, :, part] = (mine[g, :, :, part] + pair_in[g, :, :, part].astype(F32)).astype(BF16)
        for d in range(chips - 1, 0, -1):
            col_copy(n, d).start()

    def facet_sum(n):
        g, v0, width = plan[n]
        part = pl.ds(v0, width)
        wait_bytes(others.at[g, :, :, part], col_recv.at[n])
        total = mine[g, chip, :, part] + pair_in[g, chip, :, part].astype(F32)
        for d in range(1, chips):
            total = total + others[g, d - 1, :, part].astype(F32)
        gathered[g, me_row, :, part] = total.astype(BF16)
        each_inner_row(lambda target: row_copy(n, target).start())

    def row_start(at, block_row):
        column0 = (facet_off[1, facet_order[me_col]] + block_row * block_cols) & (NG - 1)
        shape = (m // FINE, block_cols)
        real, imag = cis(iota(shape, 0) * FINE * (column0 + iota(shape, 1)))
        coarse2[at, 0] = real
        coarse2[at, 1] = imag
        shape = (FINE, block_cols)
        real, imag = cis(iota(shape, 0) * (column0 + iota(shape, 1)))
        fine2[at, 0] = real
        fine2[at, 1] = imag
        row_ids = iota((rows, block_cols), 0)
        offsets = jnp.zeros((rows, block_cols), jnp.int32)
        for r in range(rows):
            offsets = jnp.where(row_ids == r, row_off[r], offsets)
        lanes = iota((rows, block_cols), 1)
        beam = 1.0 - BEAM_SLOPE * ((block_row * block_cols + lanes).astype(F32) + 0.5) / FS
        gain = (0.5 / math.sqrt(m * rows)) / beam
        real, imag = cis(offsets * ((column0 + lanes) & (NG - 1)))
        phases[at, 0] = real * gain
        phases[at, 1] = imag * gain

    def row_fill(at, first, last):
        def fill(h, carry):
            a, b = coarse2[at, 0, pl.ds(h, 1), :], coarse2[at, 1, pl.ds(h, 1), :]
            c, d = fine2[at, 0], fine2[at, 1]
            out = pl.ds(pl.multiple_of(h * FINE, FINE), FINE)
            table2[at, 0, out, :] = (a * c - b * d).astype(BF16)
            table2[at, 1, out, :] = (a * d + b * c).astype(BF16)
            return carry

        lax.fori_loop(first, last, fill, 0)

    def second(g, at):
        strongest = best[...]
        for p in range(block_cols // piece):
            part = pl.ds(p * piece, piece)
            sides = []
            for side in range(2):
                left = gathered[g].reshape(rows * 2 * group, m)
                product = dot(left, table2[at, side, :, part])
                sides.append(product.reshape(rows, 2, group, piece))
            out_real = jnp.zeros((group, piece), F32)
            out_imag = jnp.zeros((group, piece), F32)
            for r in range(rows):
                real = sides[0][r, 0] - sides[1][r, 1]
                imag = sides[1][r, 0] + sides[0][r, 1]
                a, b = phases[at, 0, pl.ds(r, 1), part], phases[at, 1, pl.ds(r, 1), part]
                out_real = out_real + (real * a - imag * b)
                out_imag = out_imag + (real * b + imag * a)
            if at == 0:
                image[0, 0, pl.ds(g * group, group), part] = out_real
                image[0, 1, pl.ds(g * group, group), part] = out_imag
            else:
                relay_out[g, p, pl.ds(0, group), :] = out_real.astype(BF16)
                relay_out[g, p, pl.ds(group, group), :] = out_imag.astype(BF16)
                relay_copy(g, p).start()
            power = out_real * out_real + out_imag * out_imag
            power = jnp.max(power.reshape(group // 8, 8, piece), axis=0)
            for lane in range(0, piece, 128):
                strongest = jnp.maximum(strongest, power[:, lane : lane + 128])
        best[...] = strongest

    def when(condition, name, act, *args):
        @pl.when(condition)
        def _():
            with jax.named_scope(name):
                act(*args)

    def arrive(g):
        wait_bytes(gathered.at[g, pl.ds(0, rows - 1)], row_recv.at[g])

    def scoped(name, act, *args):
        with jax.named_scope(name):
            act(*args)

    def T(n):
        if plan[n][1] == 0:
            scoped(f"table{n}", column_table, plan[n][0])
        scoped(f"tr{n}", transform, n)
        if n == 0:
            scoped("barrier", pl.semaphore_wait, barrier, chips + rows - 1)
        pair_copy(n).start()

    def P(n):
        scoped(f"pair{n}", pair_sum, n)

    def F(n):
        scoped(f"facet{n}", facet_sum, n)

    def R(at):
        when(inner if at == 0 else helps, f"start{at}", row_start, at, me_row if at == 0 else end_row)

    def B(step):
        at, quarter = step // 4, step % 4
        fills = m // FINE // 4
        when(inner if at == 0 else helps, f"fill{step}", row_fill, at, quarter * fills, (quarter + 1) * fills)

    def E(g):
        when(inner, f"arrive{g}", arrive, g)
        when(helps, f"second{g}1", second, g, 1)

    def S(g):
        when(inner, f"second{g}0", second, g, 0)

    steps = {"T": T, "P": P, "F": F, "R": R, "B": B, "E": E, "S": S}
    for part in ORDER:
        for step in part.split():
            steps[step[0]](int(step[1:]))

    @pl.when(inner)
    def _():
        peaks[me_row] = jnp.sqrt(best[...])
        for d in range(1, rows):
            peak_copy(peer_row(d)).start()

    @pl.when(outer)
    def _():
        for g in range(GROUPS):
            with jax.named_scope(f"relay{g}"):
                wait_bytes(relay_in.at[g], relay_recv.at[g])
                for p in range(block_cols // piece):
                    for ri in range(2):
                        here = relay_in[g, p, pl.ds(ri * group, group), :]
                        image[0, ri, pl.ds(g * group, group), pl.ds(p * piece, piece)] = here.astype(F32)

    with jax.named_scope("sends"):
        wait_bytes(pair_out, pair_send)
        wait_bytes(others, col_send)

        @pl.when(outer)
        def _():
            wait_bytes(gathered.at[:, pl.ds(0, rows - 2)], row_send)

        @pl.when(inner)
        def _():
            wait_bytes(gathered.at[:, pl.ds(0, rows - 3)], row_send)

        @pl.when(helps)
        def _():
            wait_bytes(relay_out, relay_send)

    with jax.named_scope("peakwait"):
        @pl.when(outer)
        def _():
            wait_bytes(peaks.at[pl.ds(0, rows - 2)], peak_recv)

        @pl.when(inner)
        def _():
            wait_bytes(peaks.at[pl.ds(0, rows - 3)], peak_recv)
            wait_bytes(peaks.at[pl.ds(0, rows - 1)], peak_send)

        strongest = peaks[1]
        for r in range(2, rows - 1):
            strongest = jnp.maximum(strongest, peaks[r])
        peak[0] = jnp.max(strongest)


def local(cols, rows, visibilities, col_offsets, row_offsets, facet_offsets, facet_order, vis_counts):
    m = visibilities.shape[1]
    plan = chunk_plan(m)
    chunks = len(plan)
    strips = sum(g == 0 for g, _, _ in plan)
    group = FR // GROUPS
    chips = cols // 2
    block_cols = FS // rows
    piece = min(512, block_cols)

    def blocks(lead, dtype):
        return pltpu.VMEM((GROUPS, lead, 2 * group, m), dtype)

    dma = pltpu.SemaphoreType.DMA
    smem = pl.BlockSpec(memory_space=pltpu.SMEM)
    anywhere = pl.BlockSpec(memory_space=pl.ANY)
    small = (col_offsets, row_offsets, facet_offsets.T, facet_order, vis_counts)
    return pl.pallas_call(
        functools.partial(kernel, cols, rows, plan),
        out_shape=(
            pltpu.VMEM((1, 2, FR, block_cols), F32),
            pltpu.SMEM((1,), F32),
        ),
        in_specs=[anywhere] * 6,
        out_specs=(pl.BlockSpec(memory_space=pltpu.VMEM), smem),
        scratch_shapes=[pltpu.SMEM(x.shape, x.dtype) for x in small] + [
            dma((len(small),)),
            pltpu.VMEM((2, m, m), BF16),
            pltpu.VMEM((2, cols, m), F32),
            pltpu.VMEM((2, FR, m), F32),
            pltpu.VMEM((GROUPS, 3 * cols * group, m), BF16),
            blocks(chips, F32),
            blocks(chips, BF16),
            blocks(chips, BF16),
            blocks(chips, BF16),
            blocks(chips - 1, BF16),
            blocks(rows, BF16),
            pltpu.VMEM((2, 2, m // FINE, block_cols), F32),
            pltpu.VMEM((2, 2, FINE, block_cols), F32),
            pltpu.VMEM((2, 2, m, block_cols), BF16),
            pltpu.VMEM((2, 2, rows, block_cols), F32),
            pltpu.VMEM((GROUPS, block_cols // piece, 2 * group, piece), BF16),
            pltpu.VMEM((GROUPS, block_cols // piece, 2 * group, piece), BF16),
            pltpu.VMEM((8, 128), F32),
            pltpu.VMEM((rows, 8, 128), F32),
            dma((strips,)),
            dma,
            dma((chunks,)),
            dma,
            dma((chunks,)),
            dma,
            dma((GROUPS,)),
            dma,
            dma((GROUPS,)),
            dma,
            dma,
        ],
        compiler_params=pltpu.CompilerParams(
            collective_id=0, has_side_effects=True, vmem_limit_bytes=60 * 1024 * 1024),
    )(visibilities, *small)


def solution(mesh):
    in_specs = (P(None, "col", "row"), P("col"), P(), P(), P(), P("col", "row"))
    out_specs = (P("col", None, None, "row"), P("col"))
    body = functools.partial(local, mesh.shape["col"], mesh.shape["row"])
    return jax.shard_map(body, mesh=mesh, in_specs=in_specs, out_specs=out_specs, check_vma=False)
```

```python
import functools
import math

import jax
import jax.numpy as jnp
from jax import lax
from jax.experimental import pallas as pl
from jax.experimental.pallas import tpu as pltpu
from jax.sharding import PartitionSpec as P

FS = 4096
NG = 16384
FR = 64
TWO_PI = 2.0 * math.pi
BEAM_SLOPE = 0.66
FINE = 32
GROUPS = 4
ORDER = (
    "T0", "T1", "R0", "P0", "N0", "T2", "P1", "N1", "T3", "B0", "B1", "P2", "T4", "P3", "N2", "T5", "P4", "N3",
    "F0", "T6", "F1", "P5", "N4", "T7", "F2", "T8", "P6", "N5", "B2", "B3", "F3", "T9", "P7", "N6", "P8", "N7",
    "R1", "B4", "F4", "P9", "N8", "N9", "B5", "B6", "B7", "F5", "E0", "F6", "S0", "F7", "E1", "F8", "F9", "S1",
    "E2", "S2", "H0", "H1", "E3", "S3",
)
MESH = pl.DeviceIdType.MESH
F32 = jnp.float32
BF16 = jnp.bfloat16


def cis(product):
    shift = (NG // 4).bit_length() - 1
    turn = product & (NG - 1)
    quadrant = (turn + NG // 8) >> shift
    rest = turn - (quadrant << shift)
    angle = rest.astype(F32) * (TWO_PI / NG)
    z = angle * angle
    sine = angle * (1.0 + z * (-1.0 / 6 + z * (1.0 / 120 + z * (-1.0 / 5040 + z * (1.0 / 362880)))))
    cosine = 1.0 + z * (-0.5 + z * (1.0 / 24 + z * (-1.0 / 720 + z * (1.0 / 40320))))
    odd = (quadrant & 1) == 1
    real = jnp.where(odd, sine, cosine)
    imag = jnp.where(odd, cosine, sine)
    real = jnp.where(((quadrant + 1) & 2) != 0, -real, real)
    imag = jnp.where((quadrant & 2) != 0, -imag, imag)
    return real, imag


def iota(shape, dim):
    return lax.broadcasted_iota(jnp.int32, shape, dim)


def chunk_plan(m):
    half, quarter = m // 2, m // 4
    plan = []
    for g in range(GROUPS):
        for h in range(2):
            if (g, h) in ((0, 0), (GROUPS - 1, 1)):
                plan += [(g, h * half, quarter), (g, h * half + quarter, quarter)]
            else:
                plan.append((g, h * half, half))
    return plan


def kernel(
    cols, rows, plan,
    vis_hbm, *refs,
):
    small, (image, peak), scratch = refs[:5], refs[5:7], refs[7:]
    (
    col_off, row_off, facet_off, facet_order, counts, small_sem,
    vis, head, fine, table, mine, pair_out, pair_in, sums, others, gathered,
    coarse2, fine2, table2, phases, relay_out, relay_in, early, best, peaks,
    vis_sem, pair_send, pair_recv, col_send, col_recv, row_send, row_recv,
    relay_send, relay_recv, peak_send, peak_recv,
    ) = scratch
    copies = [
        pltpu.make_async_copy(source, target, small_sem.at[n])
        for n, (source, target) in enumerate(zip(small, scratch[:5]))
    ]
    for copy in copies:
        copy.start()
    m = vis.shape[1]
    group = FR // GROUPS
    chips = cols // 2
    block_cols = FS // rows
    piece = min(512, block_cols)
    chunks = len(plan)
    me_col = lax.axis_index("col")
    me_row = lax.axis_index("row")
    core = lax.rem(me_col, 2)
    chip = me_col // 2
    partner = chip * 2 + 1 - core
    inner = (me_row >= 1) & (me_row <= rows - 2)
    outer = (me_row == 0) | (me_row == rows - 1)
    helps = (me_row == 1) | (me_row == rows - 2)
    end_row = jnp.where(me_row <= 1, 0, rows - 1)

    def peer_chip(d):
        return lax.rem(chip + d, chips) * 2 + core

    def peer_row(d):
        return lax.rem(me_row + d, rows)

    barrier = pltpu.get_barrier_semaphore()
    pl.semaphore_signal(barrier, inc=1, device_id=(partner, me_row), device_id_type=MESH)
    for d in range(1, chips):
        pl.semaphore_signal(barrier, inc=1, device_id=(peer_chip(d), me_row), device_id_type=MESH)
    for d in range(1, rows):
        @pl.when(inner | ((peer_row(d) >= 1) & (peer_row(d) <= rows - 2)))
        def _():
            pl.semaphore_signal(barrier, inc=1, device_id=(me_col, peer_row(d)), device_id_type=MESH)

    strips = [(v0, width) for g, v0, width in plan if g == 0]

    def vis_copy(h):
        part = pl.ds(*strips[h])
        return pltpu.make_async_copy(vis_hbm.at[:, :, part], vis.at[:, :, part], vis_sem.at[h])

    for h in range(len(strips)):
        vis_copy(h).start()

    real, imag = cis(iota((FR, m), 0) * iota((FR, m), 1))
    fine[0] = real
    fine[1] = imag
    best[...] = jnp.zeros(best.shape, F32)

    with jax.named_scope("small"):
        for copy in copies:
            copy.wait()

    u = iota((cols, m), 1)
    slot = iota((cols, m), 0)
    start = jnp.zeros((cols, m), jnp.int32)
    for half in range(2):
        for c in range(chips):
            facet = facet_order[c * 2 + (core if half == 0 else 1 - core)]
            first = (facet_off[0, facet] + (FS // 2 - FR // 2)) & (NG - 1)
            start = jnp.where(slot == half * chips + c, first, start)
    real, imag = cis(start * (col_off[0] + u))
    scale = jnp.where(u < counts[0, 0], 1.0 / math.sqrt(m * cols), 0.0)
    head[0] = real * scale
    head[1] = imag * scale
    turns = cis(iota((FR, 128), 0) * col_off[0])
    block = cols * group
    dot = functools.partial(jnp.dot, preferred_element_type=F32)

    def column_table(g):
        rows_here = slice(g * group, (g + 1) * group)
        a, b = (jnp.concatenate([x[rows_here]] * (m // 128), axis=1) for x in turns)
        c, d = fine[0, rows_here, :], fine[1, rows_here, :]
        c, d = a * c - b * d, a * d + b * c
        for s in range(cols):
            a, b = head[0, pl.ds(s, 1), :], head[1, pl.ds(s, 1), :]
            imag = a * d + b * c
            real = a * c - b * d
            table[g, pl.ds(s * group, group), :] = real.astype(BF16)
            table[g, pl.ds(block + s * group, group), :] = imag.astype(BF16)
            table[g, pl.ds(2 * block + s * group, group), :] = (-real).astype(BF16)

    def pair_copy(n):
        g, v0, width = plan[n]
        part = pl.ds(v0, width)
        return pltpu.make_async_remote_copy(
            src_ref=pair_out.at[g, :, :, part], dst_ref=pair_in.at[g, :, :, part],
            send_sem=pair_send, recv_sem=pair_recv.at[n],
            device_id=(partner, me_row), device_id_type=MESH)

    def col_copy(n, target):
        g, v0, width = plan[n]
        part = pl.ds(v0, width)
        return pltpu.make_async_remote_copy(
            src_ref=sums.at[g, target, :, part], dst_ref=others.at[g, chip, :, part],
            send_sem=col_send, recv_sem=col_recv.at[n],
            device_id=(target * 2 + core, me_row), device_id_type=MESH)

    def row_copy(n, target):
        g, v0, width = plan[n]
        part = pl.ds(v0, width)
        return pltpu.make_async_remote_copy(
            src_ref=gathered.at[g, me_row, :, part], dst_ref=gathered.at[g, me_row, :, part],
            send_sem=row_send, recv_sem=row_recv.at[g + (g == GROUPS - 1 and v0 >= m // 2)],
            device_id=(me_col, target), device_id_type=MESH)

    def relay_copy(g, p):
        return pltpu.make_async_remote_copy(
            src_ref=relay_out.at[g, p], dst_ref=relay_in.at[g, p],
            send_sem=relay_send, recv_sem=relay_recv.at[g],
            device_id=(me_col, end_row), device_id_type=MESH)

    def peak_copy(target):
        return pltpu.make_async_remote_copy(
            src_ref=peaks.at[me_row], dst_ref=peaks.at[me_row],
            send_sem=peak_send, recv_sem=peak_recv,
            device_id=(me_col, target), device_id_type=MESH)

    def wait_bytes(ref, sem):
        pltpu.make_async_copy(ref, ref, sem).wait()

    def each_inner_row(act):
        for dist in range(rows - 1, 0, -1):
            for step in (dist, -dist):
                target = me_row + step

                @pl.when((target >= 1) & (target <= rows - 2))
                def _():
                    act(target)

    def transform(n):
        g, v0, width = plan[n]
        part = pl.ds(v0, width)
        if g == 0:
            vis_copy(n).wait()
        both = dot(table[g, pl.ds(0, 2 * block), :], vis[0, :, part])
        both = both - dot(table[g, pl.ds(block, 2 * block), :], vis[1, :, part])
        both = both.reshape(2, 2, chips, group, width)
        for ri in range(2):
            pair_out[g, :, pl.ds(ri * group, group), part] = both[ri, 1].astype(BF16)
            mine[g, :, pl.ds(ri * group, group), part] = both[ri, 0]

    def pair_sum(n):
        pair_copy(n).wait_recv()
        g, v0, width = plan[n]
        part = pl.ds(v0, width)
        sums[g, :, :, part] = (mine[g, :, :, part] + pair_in[g, :, :, part].astype(F32)).astype(BF16)

    def col_start(n):
        for target in range(chips):
            @pl.when(target != chip)
            def _():
                col_copy(n, target).start()

    def facet_sum(n):
        g, v0, width = plan[n]
        part = pl.ds(v0, width)
        wait_bytes(others.at[g, pl.ds(0, chips - 1), :, part], col_recv.at[n])
        total = mine[g, chip, :, part] + pair_in[g, chip, :, part].astype(F32)
        for d in range(1, chips):
            total = total + others[g, lax.rem(chip + d, chips), :, part].astype(F32)
        gathered[g, me_row, :, part] = total.astype(BF16)
        each_inner_row(lambda target: row_copy(n, target).start())

    def row_start(at, block_row):
        column0 = (facet_off[1, facet_order[me_col]] + block_row * block_cols) & (NG - 1)
        shape = (m // FINE, block_cols)
        real, imag = cis(iota(shape, 0) * FINE * (column0 + iota(shape, 1)))
        coarse2[at, 0] = real
        coarse2[at, 1] = imag
        shape = (FINE, block_cols)
        real, imag = cis(iota(shape, 0) * (column0 + iota(shape, 1)))
        fine2[at, 0] = real
        fine2[at, 1] = imag
        row_ids = iota((rows, block_cols), 0)
        offsets = jnp.zeros((rows, block_cols), jnp.int32)
        for r in range(rows):
            offsets = jnp.where(row_ids == r, row_off[r], offsets)
        lanes = iota((rows, block_cols), 1)
        beam = 1.0 - BEAM_SLOPE * ((block_row * block_cols + lanes).astype(F32) + 0.5) / FS
        gain = (0.5 / math.sqrt(m * rows)) / beam
        real, imag = cis(offsets * ((column0 + lanes) & (NG - 1)))
        phases[at, 0] = real * gain
        phases[at, 1] = imag * gain

    def row_fill(at, first, last):
        def fill(h, carry):
            a, b = coarse2[at, 0, pl.ds(h, 1), :], coarse2[at, 1, pl.ds(h, 1), :]
            c, d = fine2[at, 0], fine2[at, 1]
            out = pl.ds(pl.multiple_of(h * FINE, FINE), FINE)
            table2[at, 0, out, :] = (a * c - b * d).astype(BF16)
            table2[at, 1, out, :] = (a * d + b * c).astype(BF16)
            return carry

        lax.fori_loop(first, last, fill, 0)

    def second(g, at):
        strongest = best[...]
        for p in range(block_cols // piece):
            part = pl.ds(p * piece, piece)
            sides = []
            for side in range(2):
                v0 = m // 2 if g == GROUPS - 1 else 0
                left = gathered[g, :, :, pl.ds(v0, m - v0)].reshape(rows * 2 * group, m - v0)
                product = dot(left, table2[at, side, pl.ds(v0, m - v0), part])
                if v0:
                    product = product + early[at, side, :, part]
                sides.append(product.reshape(rows, 2, group, piece))
            out_real = jnp.zeros((group, piece), F32)
            out_imag = jnp.zeros((group, piece), F32)
            for r in range(rows):
                real = sides[0][r, 0] - sides[1][r, 1]
                imag = sides[1][r, 0] + sides[0][r, 1]
                a, b = phases[at, 0, pl.ds(r, 1), part], phases[at, 1, pl.ds(r, 1), part]
                out_real = out_real + (real * a - imag * b)
                out_imag = out_imag + (real * b + imag * a)
            if at == 0:
                image[0, 0, pl.ds(g * group, group), part] = out_real
                image[0, 1, pl.ds(g * group, group), part] = out_imag
            else:
                relay_out[g, p, pl.ds(0, group), :] = out_real.astype(BF16)
                relay_out[g, p, pl.ds(group, group), :] = out_imag.astype(BF16)
                relay_copy(g, p).start()
            power = out_real * out_real + out_imag * out_imag
            power = jnp.max(power.reshape(group // 8, 8, piece), axis=0)
            for lane in range(0, piece, 128):
                strongest = jnp.maximum(strongest, power[:, lane : lane + 128])
        best[...] = strongest

    def first_half(at):
        left = gathered[GROUPS - 1, :, :, pl.ds(0, m // 2)].reshape(rows * 2 * group, m // 2)
        for side in range(2):
            early[at, side] = dot(left, table2[at, side, pl.ds(0, m // 2), :])

    def when(condition, name, act, *args):
        @pl.when(condition)
        def _():
            with jax.named_scope(name):
                act(*args)

    def arrive(g):
        late = g == GROUPS - 1
        part = pl.ds(m // 2, m // 2) if late else pl.ds(0, m)
        wait_bytes(gathered.at[g, pl.ds(0, rows - 1), :, part], row_recv.at[g + late])

    def arrive_half():
        wait_bytes(gathered.at[GROUPS - 1, pl.ds(0, rows - 1), :, pl.ds(0, m // 2)], row_recv.at[GROUPS - 1])

    def scoped(name, act, *args):
        with jax.named_scope(name):
            act(*args)

    def T(n):
        if plan[n][1] == 0:
            scoped(f"table{n}", column_table, plan[n][0])
        scoped(f"tr{n}", transform, n)
        if n == 0:
            when(inner, "barrier", pl.semaphore_wait, barrier, chips + rows - 1)
            when(outer, "barrier", pl.semaphore_wait, barrier, chips + rows - 2)
        pair_copy(n).start()

    def P(n):
        scoped(f"pair{n}", pair_sum, n)
        when(core == 0, f"col{n}", col_start, n)

    def N(n):
        when(core == 1, f"col{n}", col_start, n)

    def F(n):
        scoped(f"facet{n}", facet_sum, n)

    def R(at):
        when(inner if at == 0 else helps, f"start{at}", row_start, at, me_row if at == 0 else end_row)

    def B(step):
        at, quarter = step // 4, step % 4
        fills = m // FINE // 4
        when(inner if at == 0 else helps, f"fill{step}", row_fill, at, quarter * fills, (quarter + 1) * fills)

    def E(g):
        when(inner, f"arrive{g}", arrive, g)
        when(helps, f"second{g}1", second, g, 1)

    def H(step):
        if step == 0:
            when(inner, "arrivehalf", arrive_half)
            when(helps, "half1", first_half, 1)
        else:
            when(inner, "half0", first_half, 0)

    def S(g):
        when(inner, f"second{g}0", second, g, 0)

    steps = {"T": T, "P": P, "N": N, "F": F, "R": R, "B": B, "E": E, "H": H, "S": S}
    for step in ORDER:
        steps[step[0]](int(step[1:]))

    @pl.when(inner)
    def _():
        peaks[me_row] = jnp.sqrt(best[...])
        for d in range(1, rows):
            peak_copy(peer_row(d)).start()

    @pl.when(outer)
    def _():
        for g in range(GROUPS):
            with jax.named_scope(f"relay{g}"):
                wait_bytes(relay_in.at[g], relay_recv.at[g])
                for p in range(block_cols // piece):
                    for ri in range(2):
                        here = relay_in[g, p, pl.ds(ri * group, group), :]
                        image[0, ri, pl.ds(g * group, group), pl.ds(p * piece, piece)] = here.astype(F32)

    with jax.named_scope("sends"):
        wait_bytes(pair_out, pair_send)
        wait_bytes(others.at[:, pl.ds(0, chips - 1)], col_send)

        @pl.when(outer)
        def _():
            wait_bytes(gathered.at[:, pl.ds(0, rows - 2)], row_send)

        @pl.when(inner)
        def _():
            wait_bytes(gathered.at[:, pl.ds(0, rows - 3)], row_send)

        @pl.when(helps)
        def _():
            wait_bytes(relay_out, relay_send)

    with jax.named_scope("peakwait"):
        @pl.when(outer)
        def _():
            wait_bytes(peaks.at[pl.ds(0, rows - 2)], peak_recv)

        @pl.when(inner)
        def _():
            wait_bytes(peaks.at[pl.ds(0, rows - 3)], peak_recv)
            wait_bytes(peaks.at[pl.ds(0, rows - 1)], peak_send)

        strongest = peaks[1]
        for r in range(2, rows - 1):
            strongest = jnp.maximum(strongest, peaks[r])
        peak[0] = jnp.max(strongest)


def local(cols, rows, visibilities, col_offsets, row_offsets, facet_offsets, facet_order, vis_counts):
    m = visibilities.shape[1]
    plan = chunk_plan(m)
    chunks = len(plan)
    strips = sum(g == 0 for g, _, _ in plan)
    group = FR // GROUPS
    chips = cols // 2
    block_cols = FS // rows
    piece = min(512, block_cols)

    def blocks(lead, dtype):
        return pltpu.VMEM((GROUPS, lead, 2 * group, m), dtype)

    dma = pltpu.SemaphoreType.DMA
    smem = pl.BlockSpec(memory_space=pltpu.SMEM)
    anywhere = pl.BlockSpec(memory_space=pl.ANY)
    small = (col_offsets, row_offsets, facet_offsets.T, facet_order, vis_counts)
    return pl.pallas_call(
        functools.partial(kernel, cols, rows, plan),
        out_shape=(
            pltpu.VMEM((1, 2, FR, block_cols), F32),
            pltpu.SMEM((1,), F32),
        ),
        in_specs=[anywhere] * 6,
        out_specs=(pl.BlockSpec(memory_space=pltpu.VMEM), smem),
        scratch_shapes=[pltpu.SMEM(x.shape, x.dtype) for x in small] + [
            dma((len(small),)),
            pltpu.VMEM((2, m, m), BF16),
            pltpu.VMEM((2, cols, m), F32),
            pltpu.VMEM((2, FR, m), F32),
            pltpu.VMEM((GROUPS, 3 * cols * group, m), BF16),
            blocks(chips, F32),
            blocks(chips, BF16),
            blocks(chips, BF16),
            blocks(chips, BF16),
            blocks(chips, BF16),
            blocks(rows, BF16),
            pltpu.VMEM((2, 2, m // FINE, block_cols), F32),
            pltpu.VMEM((2, 2, FINE, block_cols), F32),
            pltpu.VMEM((2, 2, m, block_cols), BF16),
            pltpu.VMEM((2, 2, rows, block_cols), F32),
            pltpu.VMEM((GROUPS, block_cols // piece, 2 * group, piece), BF16),
            pltpu.VMEM((GROUPS, block_cols // piece, 2 * group, piece), BF16),
            pltpu.VMEM((2, 2, rows * 2 * group, block_cols), F32),
            pltpu.VMEM((8, 128), F32),
            pltpu.VMEM((rows, 8, 128), F32),
            dma((strips,)),
            dma,
            dma((chunks,)),
            dma,
            dma((chunks,)),
            dma,
            dma((GROUPS + 1,)),
            dma,
            dma((GROUPS,)),
            dma,
            dma,
        ],
        compiler_params=pltpu.CompilerParams(
            collective_id=0, has_side_effects=True, vmem_limit_bytes=60 * 1024 * 1024),
    )(visibilities, *small)


def solution(mesh):
    in_specs = (P(None, "col", "row"), P("col"), P(), P(), P(), P("col", "row"))
    out_specs = (P("col", None, None, "row"), P("col"))
    body = functools.partial(local, mesh.shape["col"], mesh.shape["row"])
    return jax.shard_map(body, mesh=mesh, in_specs=in_specs, out_specs=out_specs, check_vma=False)
```

```python
import functools
import math

import jax
import jax.numpy as jnp
from jax import lax
from jax.experimental import pallas as pl
from jax.experimental.pallas import tpu as pltpu
from jax.sharding import PartitionSpec as P

FS = 4096
NG = 16384
FR = 64
TWO_PI = 2.0 * math.pi
BEAM_SLOPE = 0.66
FINE = 32
GROUPS = 4
ORDER = (
    "T0", "T1", "R0", "P0", "N0", "T2", "P1", "N1", "T3", "B0", "B1", "P2", "T4", "P3", "N2", "T5", "P4", "N3",
    "F0", "T6", "F1", "P5", "N4", "T7", "F2", "T8", "P6", "N5", "B2", "B3", "F3", "T9", "P7", "N6", "P8", "N7",
    "R1", "B4", "F4", "P9", "N8", "N9", "B5", "B6", "B7", "F5", "E0", "F6", "S0", "F7", "E1", "F8", "F9", "S1",
    "E2", "S2", "H0", "H1", "E3", "S3",
)
MESH = pl.DeviceIdType.MESH
F32 = jnp.float32
BF16 = jnp.bfloat16


def cis(product):
    shift = (NG // 4).bit_length() - 1
    turn = product & (NG - 1)
    quadrant = (turn + NG // 8) >> shift
    rest = turn - (quadrant << shift)
    angle = rest.astype(F32) * (TWO_PI / NG)
    z = angle * angle
    sine = angle * (1.0 + z * (-1.0 / 6 + z * (1.0 / 120 + z * (-1.0 / 5040 + z * (1.0 / 362880)))))
    cosine = 1.0 + z * (-0.5 + z * (1.0 / 24 + z * (-1.0 / 720 + z * (1.0 / 40320))))
    odd = (quadrant & 1) == 1
    real = jnp.where(odd, sine, cosine)
    imag = jnp.where(odd, cosine, sine)
    real = jnp.where(((quadrant + 1) & 2) != 0, -real, real)
    imag = jnp.where((quadrant & 2) != 0, -imag, imag)
    return real, imag


def iota(shape, dim):
    return lax.broadcasted_iota(jnp.int32, shape, dim)


def chunk_plan(m):
    half, quarter = m // 2, m // 4
    plan = []
    for g in range(GROUPS):
        for h in range(2):
            if (g, h) in ((0, 0), (GROUPS - 1, 1)):
                plan += [(g, h * half, quarter), (g, h * half + quarter, quarter)]
            else:
                plan.append((g, h * half, half))
    return plan


def kernel(
    cols, rows, plan,
    vis_hbm, *refs,
):
    small, (image, peaks), scratch = refs[:5], refs[5:7], refs[7:]
    (
    col_off, row_off, facet_off, facet_order, counts, small_sem,
    vis, head, fine, table, mine, pair_out, pair_in, sums, others, gathered,
    coarse2, fine2, table2, phases, relay_out, relay_in, early, best,
    vis_sem, pair_send, pair_recv, col_send, col_recv, row_send, row_recv,
    relay_send, relay_recv, peak_send, peak_recv,
    ) = scratch
    copies = [
        pltpu.make_async_copy(source, target, small_sem.at[n])
        for n, (source, target) in enumerate(zip(small, scratch[:5]))
    ]
    for copy in copies:
        copy.start()
    m = vis.shape[1]
    group = FR // GROUPS
    chips = cols // 2
    block_cols = FS // rows
    piece = min(512, block_cols)
    chunks = len(plan)
    me_col = lax.axis_index("col")
    me_row = lax.axis_index("row")
    core = lax.rem(me_col, 2)
    chip = me_col // 2
    partner = chip * 2 + 1 - core
    inner = (me_row >= 1) & (me_row <= rows - 2)
    outer = (me_row == 0) | (me_row == rows - 1)
    helps = (me_row == 1) | (me_row == rows - 2)
    end_row = jnp.where(me_row <= 1, 0, rows - 1)

    def peer_chip(d):
        return lax.rem(chip + d, chips) * 2 + core

    def peer_row(d):
        return lax.rem(me_row + d, rows)

    barrier = pltpu.get_barrier_semaphore()
    pl.semaphore_signal(barrier, inc=1, device_id=(partner, me_row), device_id_type=MESH)
    for d in range(1, chips):
        pl.semaphore_signal(barrier, inc=1, device_id=(peer_chip(d), me_row), device_id_type=MESH)
    for d in range(1, rows):
        @pl.when(inner | ((peer_row(d) >= 1) & (peer_row(d) <= rows - 2)))
        def _():
            pl.semaphore_signal(barrier, inc=1, device_id=(me_col, peer_row(d)), device_id_type=MESH)

    strips = [(v0, width) for g, v0, width in plan if g == 0]

    def vis_copy(h):
        part = pl.ds(*strips[h])
        return pltpu.make_async_copy(vis_hbm.at[:, :, part], vis.at[:, :, part], vis_sem.at[h])

    for h in range(len(strips)):
        vis_copy(h).start()

    real, imag = cis(iota((FR, m), 0) * iota((FR, m), 1))
    fine[0] = real
    fine[1] = imag
    best[...] = jnp.zeros(best.shape, F32)

    with jax.named_scope("small"):
        for copy in copies:
            copy.wait()

    u = iota((cols, m), 1)
    slot = iota((cols, m), 0)
    start = jnp.zeros((cols, m), jnp.int32)
    for half in range(2):
        for c in range(chips):
            facet = facet_order[c * 2 + (core if half == 0 else 1 - core)]
            first = (facet_off[0, facet] + (FS // 2 - FR // 2)) & (NG - 1)
            start = jnp.where(slot == half * chips + c, first, start)
    real, imag = cis(start * (col_off[0] + u))
    scale = jnp.where(u < counts[0, 0], 1.0 / math.sqrt(m * cols), 0.0)
    head[0] = real * scale
    head[1] = imag * scale
    turns = cis(iota((FR, 128), 0) * col_off[0])
    block = cols * group
    dot = functools.partial(jnp.dot, preferred_element_type=F32)

    def column_table(g):
        rows_here = slice(g * group, (g + 1) * group)
        a, b = (jnp.concatenate([x[rows_here]] * (m // 128), axis=1) for x in turns)
        c, d = fine[0, rows_here, :], fine[1, rows_here, :]
        c, d = a * c - b * d, a * d + b * c
        for s in range(cols):
            a, b = head[0, pl.ds(s, 1), :], head[1, pl.ds(s, 1), :]
            imag = a * d + b * c
            real = a * c - b * d
            table[g, pl.ds(s * group, group), :] = real.astype(BF16)
            table[g, pl.ds(block + s * group, group), :] = imag.astype(BF16)
            table[g, pl.ds(2 * block + s * group, group), :] = (-real).astype(BF16)

    def pair_copy(n):
        g, v0, width = plan[n]
        part = pl.ds(v0, width)
        return pltpu.make_async_remote_copy(
            src_ref=pair_out.at[g, :, :, part], dst_ref=pair_in.at[g, :, :, part],
            send_sem=pair_send, recv_sem=pair_recv.at[n],
            device_id=(partner, me_row), device_id_type=MESH)

    def col_copy(n, target):
        g, v0, width = plan[n]
        part = pl.ds(v0, width)
        return pltpu.make_async_remote_copy(
            src_ref=sums.at[g, target, :, part], dst_ref=others.at[g, chip, :, part],
            send_sem=col_send, recv_sem=col_recv.at[n],
            device_id=(target * 2 + core, me_row), device_id_type=MESH)

    def row_copy(n, target):
        g, v0, width = plan[n]
        part = pl.ds(v0, width)
        return pltpu.make_async_remote_copy(
            src_ref=gathered.at[g, me_row, :, part], dst_ref=gathered.at[g, me_row, :, part],
            send_sem=row_send, recv_sem=row_recv.at[g + (g == GROUPS - 1 and v0 >= m // 2)],
            device_id=(me_col, target), device_id_type=MESH)

    def relay_copy(g, p):
        return pltpu.make_async_remote_copy(
            src_ref=relay_out.at[g, p], dst_ref=relay_in.at[g, p],
            send_sem=relay_send, recv_sem=relay_recv.at[g],
            device_id=(me_col, end_row), device_id_type=MESH)

    def peak_copy(target):
        return pltpu.make_async_remote_copy(
            src_ref=peaks.at[me_row], dst_ref=peaks.at[me_row],
            send_sem=peak_send, recv_sem=peak_recv,
            device_id=(me_col, target), device_id_type=MESH)

    def wait_bytes(ref, sem):
        pltpu.make_async_copy(ref, ref, sem).wait()

    def each_inner_row(act):
        for dist in range(rows - 1, 0, -1):
            for step in (dist, -dist):
                target = me_row + step

                @pl.when((target >= 1) & (target <= rows - 2))
                def _():
                    act(target)

    def transform(n):
        g, v0, width = plan[n]
        part = pl.ds(v0, width)
        if g == 0:
            vis_copy(n).wait()
        both = dot(table[g, pl.ds(0, 2 * block), :], vis[0, :, part])
        both = both - dot(table[g, pl.ds(block, 2 * block), :], vis[1, :, part])
        both = both.reshape(2, 2, chips, group, width)
        for ri in range(2):
            pair_out[g, :, pl.ds(ri * group, group), part] = both[ri, 1].astype(BF16)
            mine[g, :, pl.ds(ri * group, group), part] = both[ri, 0]

    def pair_sum(n):
        pair_copy(n).wait_recv()
        g, v0, width = plan[n]
        part = pl.ds(v0, width)
        sums[g, :, :, part] = (mine[g, :, :, part] + pair_in[g, :, :, part].astype(F32)).astype(BF16)

    def col_start(n):
        for target in range(chips):
            @pl.when(target != chip)
            def _():
                col_copy(n, target).start()

    def facet_sum(n):
        g, v0, width = plan[n]
        part = pl.ds(v0, width)
        wait_bytes(others.at[g, pl.ds(0, chips - 1), :, part], col_recv.at[n])
        total = mine[g, chip, :, part] + pair_in[g, chip, :, part].astype(F32)
        for d in range(1, chips):
            total = total + others[g, lax.rem(chip + d, chips), :, part].astype(F32)
        gathered[g, me_row, :, part] = total.astype(BF16)
        each_inner_row(lambda target: row_copy(n, target).start())

    def row_start(at, block_row):
        column0 = (facet_off[1, facet_order[me_col]] + block_row * block_cols) & (NG - 1)
        shape = (m // FINE, block_cols)
        real, imag = cis(iota(shape, 0) * FINE * (column0 + iota(shape, 1)))
        coarse2[at, 0] = real
        coarse2[at, 1] = imag
        shape = (FINE, block_cols)
        real, imag = cis(iota(shape, 0) * (column0 + iota(shape, 1)))
        fine2[at, 0] = real
        fine2[at, 1] = imag
        row_ids = iota((rows, block_cols), 0)
        offsets = jnp.zeros((rows, block_cols), jnp.int32)
        for r in range(rows):
            offsets = jnp.where(row_ids == r, row_off[r], offsets)
        lanes = iota((rows, block_cols), 1)
        beam = 1.0 - BEAM_SLOPE * ((block_row * block_cols + lanes).astype(F32) + 0.5) / FS
        gain = (0.5 / math.sqrt(m * rows)) / beam
        real, imag = cis(offsets * ((column0 + lanes) & (NG - 1)))
        phases[at, 0] = real * gain
        phases[at, 1] = imag * gain

    def row_fill(at, first, last):
        def fill(h, carry):
            a, b = coarse2[at, 0, pl.ds(h, 1), :], coarse2[at, 1, pl.ds(h, 1), :]
            c, d = fine2[at, 0], fine2[at, 1]
            out = pl.ds(pl.multiple_of(h * FINE, FINE), FINE)
            table2[at, 0, out, :] = (a * c - b * d).astype(BF16)
            table2[at, 1, out, :] = (a * d + b * c).astype(BF16)
            return carry

        lax.fori_loop(first, last, fill, 0)

    def second(g, at):
        strongest = best[...]
        for p in range(block_cols // piece):
            part = pl.ds(p * piece, piece)
            sides = []
            for side in range(2):
                v0 = m // 2 if g == GROUPS - 1 else 0
                left = gathered[g, :, :, pl.ds(v0, m - v0)].reshape(rows * 2 * group, m - v0)
                product = dot(left, table2[at, side, pl.ds(v0, m - v0), part])
                if v0:
                    product = product + early[at, side, :, part]
                sides.append(product.reshape(rows, 2, group, piece))
            out_real = jnp.zeros((group, piece), F32)
            out_imag = jnp.zeros((group, piece), F32)
            for r in range(rows):
                real = sides[0][r, 0] - sides[1][r, 1]
                imag = sides[1][r, 0] + sides[0][r, 1]
                a, b = phases[at, 0, pl.ds(r, 1), part], phases[at, 1, pl.ds(r, 1), part]
                out_real = out_real + (real * a - imag * b)
                out_imag = out_imag + (real * b + imag * a)
            if at == 0:
                image[0, 0, pl.ds(g * group, group), part] = out_real
                image[0, 1, pl.ds(g * group, group), part] = out_imag
            else:
                relay_out[g, p, pl.ds(0, group), :] = out_real.astype(BF16)
                relay_out[g, p, pl.ds(group, group), :] = out_imag.astype(BF16)
            power = out_real * out_real + out_imag * out_imag
            power = jnp.max(power.reshape(group // 8, 8, piece), axis=0)
            for lane in range(0, piece, 128):
                strongest = jnp.maximum(strongest, power[:, lane : lane + 128])
        best[...] = strongest
        if at == 1:
            for p in range(block_cols // piece):
                relay_copy(g, p).start()

    def first_half(at):
        left = gathered[GROUPS - 1, :, :, pl.ds(0, m // 2)].reshape(rows * 2 * group, m // 2)
        for side in range(2):
            early[at, side] = dot(left, table2[at, side, pl.ds(0, m // 2), :])

    def when(condition, name, act, *args):
        @pl.when(condition)
        def _():
            with jax.named_scope(name):
                act(*args)

    def arrive(g):
        late = g == GROUPS - 1
        part = pl.ds(m // 2, m // 2) if late else pl.ds(0, m)
        wait_bytes(gathered.at[g, pl.ds(0, rows - 1), :, part], row_recv.at[g + late])

    def arrive_half():
        wait_bytes(gathered.at[GROUPS - 1, pl.ds(0, rows - 1), :, pl.ds(0, m // 2)], row_recv.at[GROUPS - 1])

    def scoped(name, act, *args):
        with jax.named_scope(name):
            act(*args)

    def T(n):
        if plan[n][1] == 0:
            scoped(f"table{n}", column_table, plan[n][0])
        scoped(f"tr{n}", transform, n)
        if n == 0:
            when(inner, "barrier", pl.semaphore_wait, barrier, chips + rows - 1)
            when(outer, "barrier", pl.semaphore_wait, barrier, chips + rows - 2)
        pair_copy(n).start()

    def P(n):
        scoped(f"pair{n}", pair_sum, n)
        when(core == 0, f"col{n}", col_start, n)

    def N(n):
        when(core == 1, f"col{n}", col_start, n)

    def F(n):
        scoped(f"facet{n}", facet_sum, n)

    def R(at):
        when(inner if at == 0 else helps, f"start{at}", row_start, at, me_row if at == 0 else end_row)

    def B(step):
        at, quarter = step // 4, step % 4
        fills = m // FINE // 4
        when(inner if at == 0 else helps, f"fill{step}", row_fill, at, quarter * fills, (quarter + 1) * fills)

    def E(g):
        when(inner, f"arrive{g}", arrive, g)
        when(helps, f"second{g}1", second, g, 1)

    def H(step):
        if step == 0:
            when(inner, "arrivehalf", arrive_half)
            when(helps, "half1", first_half, 1)
        else:
            when(inner, "half0", first_half, 0)

    def S(g):
        when(inner, f"second{g}0", second, g, 0)

    steps = {"T": T, "P": P, "N": N, "F": F, "R": R, "B": B, "E": E, "H": H, "S": S}
    for step in ORDER:
        steps[step[0]](int(step[1:]))

    @pl.when(inner)
    def _():
        peaks[me_row] = jnp.sqrt(best[...])
        for d in range(1, rows):
            peak_copy(peer_row(d)).start()

    @pl.when(outer)
    def _():
        for g in range(GROUPS):
            with jax.named_scope(f"relay{g}"):
                wait_bytes(relay_in.at[g], relay_recv.at[g])
                for p in range(block_cols // piece):
                    for ri in range(2):
                        here = relay_in[g, p, pl.ds(ri * group, group), :]
                        image[0, ri, pl.ds(g * group, group), pl.ds(p * piece, piece)] = here.astype(F32)

    with jax.named_scope("sends"):
        wait_bytes(pair_out, pair_send)
        wait_bytes(others.at[:, pl.ds(0, chips - 1)], col_send)

        @pl.when(outer)
        def _():
            wait_bytes(gathered.at[:, pl.ds(0, rows - 2)], row_send)

        @pl.when(inner)
        def _():
            wait_bytes(gathered.at[:, pl.ds(0, rows - 3)], row_send)

        @pl.when(helps)
        def _():
            wait_bytes(relay_out, relay_send)

    with jax.named_scope("peakwait"):
        @pl.when(outer)
        def _():
            wait_bytes(peaks.at[pl.ds(0, rows - 2)], peak_recv)

        @pl.when(inner)
        def _():
            wait_bytes(peaks.at[pl.ds(0, rows - 3)], peak_recv)
            wait_bytes(peaks.at[pl.ds(0, rows - 1)], peak_send)


def finish_kernel(rows, image, peaks, image_out, peak_out, peak, image_sem, peak_sem):
    copy = pltpu.make_async_copy(image, image_out, image_sem)
    copy.start()
    strongest = peaks[1]
    for r in range(2, rows - 1):
        strongest = jnp.maximum(strongest, peaks[r])
    peak[0] = jnp.max(strongest)
    peak_copy = pltpu.make_async_copy(peak, peak_out, peak_sem)
    peak_copy.start()
    peak_copy.wait()
    copy.wait()


def local(cols, rows, visibilities, col_offsets, row_offsets, facet_offsets, facet_order, vis_counts):
    m = visibilities.shape[1]
    plan = chunk_plan(m)
    chunks = len(plan)
    strips = sum(g == 0 for g, _, _ in plan)
    group = FR // GROUPS
    chips = cols // 2
    block_cols = FS // rows
    piece = min(512, block_cols)

    def blocks(lead, dtype):
        return pltpu.VMEM((GROUPS, lead, 2 * group, m), dtype)

    dma = pltpu.SemaphoreType.DMA
    in_vmem = pl.BlockSpec(memory_space=pltpu.VMEM)
    anywhere = pl.BlockSpec(memory_space=pl.ANY)
    small = (col_offsets, row_offsets, facet_offsets.T, facet_order, vis_counts)
    image, peaks = pl.pallas_call(
        functools.partial(kernel, cols, rows, plan),
        out_shape=(
            pltpu.VMEM((1, 2, FR, block_cols), F32),
            pltpu.VMEM((rows, 8, 128), F32),
        ),
        in_specs=[anywhere] * 6,
        out_specs=(in_vmem, in_vmem),
        scratch_shapes=[pltpu.SMEM(x.shape, x.dtype) for x in small] + [
            dma((len(small),)),
            pltpu.VMEM((2, m, m), BF16),
            pltpu.VMEM((2, cols, m), F32),
            pltpu.VMEM((2, FR, m), F32),
            pltpu.VMEM((GROUPS, 3 * cols * group, m), BF16),
            blocks(chips, F32),
            blocks(chips, BF16),
            blocks(chips, BF16),
            blocks(chips, BF16),
            blocks(chips, BF16),
            blocks(rows, BF16),
            pltpu.VMEM((2, 2, m // FINE, block_cols), F32),
            pltpu.VMEM((2, 2, FINE, block_cols), F32),
            pltpu.VMEM((2, 2, m, block_cols), BF16),
            pltpu.VMEM((2, 2, rows, block_cols), F32),
            pltpu.VMEM((GROUPS, block_cols // piece, 2 * group, piece), BF16),
            pltpu.VMEM((GROUPS, block_cols // piece, 2 * group, piece), BF16),
            pltpu.VMEM((2, 2, rows * 2 * group, block_cols), F32),
            pltpu.VMEM((8, 128), F32),
            dma((strips,)),
            dma,
            dma((chunks,)),
            dma,
            dma((chunks,)),
            dma,
            dma((GROUPS + 1,)),
            dma,
            dma((GROUPS,)),
            dma,
            dma,
        ],
        compiler_params=pltpu.CompilerParams(
            collective_id=0, has_side_effects=True, vmem_limit_bytes=60 * 1024 * 1024),
    )(visibilities, *small)
    return pl.pallas_call(
        functools.partial(finish_kernel, rows),
        out_shape=(jax.ShapeDtypeStruct(image.shape, F32), jax.ShapeDtypeStruct((1,), F32)),
        in_specs=[in_vmem, in_vmem],
        out_specs=(anywhere, anywhere),
        scratch_shapes=[pltpu.SMEM((1,), F32), dma, dma],
        compiler_params=pltpu.CompilerParams(vmem_limit_bytes=1024 * 1024),
    )(image, peaks)


def solution(mesh):
    in_specs = (P(None, "col", "row"), P("col"), P(), P(), P(), P("col", "row"))
    out_specs = (P("col", None, None, "row"), P("col"))
    body = functools.partial(local, mesh.shape["col"], mesh.shape["row"])
    return jax.shard_map(body, mesh=mesh, in_specs=in_specs, out_specs=out_specs, check_vma=False)
```

```python
import functools
import math

import jax
import jax.numpy as jnp
from jax import lax
from jax.experimental import pallas as pl
from jax.experimental.pallas import tpu as pltpu
from jax.sharding import PartitionSpec as P

FS = 4096
NG = 16384
FR = 64
TWO_PI = 2.0 * math.pi
BEAM_SLOPE = 0.66
FINE = 32
GROUPS = 4
ORDER = (
    "T0", "T1", "R0", "P0", "N0", "T2", "P1", "T3", "P2", "N1", "B0", "B1", "T4", "P3", "N2", "F0", "T5", "P4",
    "N3", "F1", "T6", "P5", "N4", "B2", "B3", "F2", "T7", "P6", "N5", "R1", "B4", "F3", "P7", "N6", "N7", "B5",
    "B6", "B7", "F4", "E0", "F5", "S0", "F6", "E1", "F7", "S1", "E2", "S2", "H0", "H1", "E3", "S3",
)
MESH = pl.DeviceIdType.MESH
F32 = jnp.float32
BF16 = jnp.bfloat16


def cis(product):
    shift = (NG // 4).bit_length() - 1
    turn = product & (NG - 1)
    quadrant = (turn + NG // 8) >> shift
    rest = turn - (quadrant << shift)
    angle = rest.astype(F32) * (TWO_PI / NG)
    z = angle * angle
    sine = angle * (1.0 + z * (-1.0 / 6 + z * (1.0 / 120 + z * (-1.0 / 5040 + z * (1.0 / 362880)))))
    cosine = 1.0 + z * (-0.5 + z * (1.0 / 24 + z * (-1.0 / 720 + z * (1.0 / 40320))))
    odd = (quadrant & 1) == 1
    real = jnp.where(odd, sine, cosine)
    imag = jnp.where(odd, cosine, sine)
    real = jnp.where(((quadrant + 1) & 2) != 0, -real, real)
    imag = jnp.where((quadrant & 2) != 0, -imag, imag)
    return real, imag


def iota(shape, dim):
    return lax.broadcasted_iota(jnp.int32, shape, dim)


def chunk_plan(m):
    half = m // 2
    plan = []
    for g in range(GROUPS):
        for h in range(2):
            plan.append((g, h * half, half))
    return plan


def kernel(
    cols, rows, plan,
    vis_hbm, *refs,
):
    small, (image, peaks), scratch = refs[:5], refs[5:7], refs[7:]
    (
    col_off, row_off, facet_off, facet_order, counts, small_sem,
    vis, head, fine, table, mine, pair_out, pair_in, sums, others, gathered,
    coarse2, fine2, table2, phases, relay_out, relay_in, early, best,
    vis_sem, pair_send, pair_recv, col_send, col_recv, row_send, row_recv,
    relay_send, relay_recv, peak_send, peak_recv,
    ) = scratch
    copies = [
        pltpu.make_async_copy(source, target, small_sem.at[n])
        for n, (source, target) in enumerate(zip(small, scratch[:5]))
    ]
    for copy in copies:
        copy.start()
    m = vis.shape[1]
    group = FR // GROUPS
    chips = cols // 2
    block_cols = FS // rows
    piece = min(512, block_cols)
    chunks = len(plan)
    me_col = lax.axis_index("col")
    me_row = lax.axis_index("row")
    core = lax.rem(me_col, 2)
    chip = me_col // 2
    partner = chip * 2 + 1 - core
    inner = (me_row >= 1) & (me_row <= rows - 2)
    outer = (me_row == 0) | (me_row == rows - 1)
    helps = (me_row == 1) | (me_row == rows - 2)
    end_row = jnp.where(me_row <= 1, 0, rows - 1)

    def peer_chip(d):
        return lax.rem(chip + d, chips) * 2 + core

    def peer_row(d):
        return lax.rem(me_row + d, rows)

    barrier = pltpu.get_barrier_semaphore()
    pl.semaphore_signal(barrier, inc=1, device_id=(partner, me_row), device_id_type=MESH)
    for d in range(1, chips):
        pl.semaphore_signal(barrier, inc=1, device_id=(peer_chip(d), me_row), device_id_type=MESH)
    for d in range(1, rows):
        @pl.when(inner | ((peer_row(d) >= 1) & (peer_row(d) <= rows - 2)))
        def _():
            pl.semaphore_signal(barrier, inc=1, device_id=(me_col, peer_row(d)), device_id_type=MESH)

    strips = [(v0, width) for g, v0, width in plan if g == 0]

    def vis_copy(h):
        part = pl.ds(*strips[h])
        return pltpu.make_async_copy(vis_hbm.at[:, :, part], vis.at[:, :, part], vis_sem.at[h])

    for h in range(len(strips)):
        vis_copy(h).start()

    real, imag = cis(iota((FR, m), 0) * iota((FR, m), 1))
    fine[0] = real
    fine[1] = imag
    best[...] = jnp.zeros(best.shape, F32)

    with jax.named_scope("small"):
        for copy in copies:
            copy.wait()

    u = iota((cols, m), 1)
    slot = iota((cols, m), 0)
    start = jnp.zeros((cols, m), jnp.int32)
    for half in range(2):
        for c in range(chips):
            facet = facet_order[c * 2 + (core if half == 0 else 1 - core)]
            first = (facet_off[0, facet] + (FS // 2 - FR // 2)) & (NG - 1)
            start = jnp.where(slot == half * chips + c, first, start)
    real, imag = cis(start * (col_off[0] + u))
    scale = jnp.where(u < counts[0, 0], 1.0 / math.sqrt(m * cols), 0.0)
    head[0] = real * scale
    head[1] = imag * scale
    turns = cis(iota((FR, 128), 0) * col_off[0])
    block = cols * group
    dot = functools.partial(jnp.dot, preferred_element_type=F32)

    def column_table(g):
        rows_here = slice(g * group, (g + 1) * group)
        a, b = (jnp.concatenate([x[rows_here]] * (m // 128), axis=1) for x in turns)
        c, d = fine[0, rows_here, :], fine[1, rows_here, :]
        c, d = a * c - b * d, a * d + b * c
        for s in range(cols):
            a, b = head[0, pl.ds(s, 1), :], head[1, pl.ds(s, 1), :]
            imag = a * d + b * c
            real = a * c - b * d
            table[g, pl.ds(s * group, group), :] = real.astype(BF16)
            table[g, pl.ds(block + s * group, group), :] = imag.astype(BF16)
            table[g, pl.ds(2 * block + s * group, group), :] = (-real).astype(BF16)

    def pair_copy(n):
        g, v0, width = plan[n]
        part = pl.ds(v0, width)
        return pltpu.make_async_remote_copy(
            src_ref=pair_out.at[g, :, :, part], dst_ref=pair_in.at[g, :, :, part],
            send_sem=pair_send, recv_sem=pair_recv.at[n],
            device_id=(partner, me_row), device_id_type=MESH)

    def col_copy(n, target):
        g, v0, width = plan[n]
        part = pl.ds(v0, width)
        return pltpu.make_async_remote_copy(
            src_ref=sums.at[g, target, :, part], dst_ref=others.at[g, chip, :, part],
            send_sem=col_send, recv_sem=col_recv.at[n],
            device_id=(target * 2 + core, me_row), device_id_type=MESH)

    def row_copy(n, target):
        g, v0, width = plan[n]
        part = pl.ds(v0, width)
        return pltpu.make_async_remote_copy(
            src_ref=gathered.at[g, me_row, :, part], dst_ref=gathered.at[g, me_row, :, part],
            send_sem=row_send, recv_sem=row_recv.at[g + (g == GROUPS - 1 and v0 >= m // 2)],
            device_id=(me_col, target), device_id_type=MESH)

    def relay_copy(g, p):
        return pltpu.make_async_remote_copy(
            src_ref=relay_out.at[g, p], dst_ref=relay_in.at[g, p],
            send_sem=relay_send, recv_sem=relay_recv.at[g],
            device_id=(me_col, end_row), device_id_type=MESH)

    def peak_copy(target):
        return pltpu.make_async_remote_copy(
            src_ref=peaks.at[me_row], dst_ref=peaks.at[me_row],
            send_sem=peak_send, recv_sem=peak_recv,
            device_id=(me_col, target), device_id_type=MESH)

    def wait_bytes(ref, sem):
        pltpu.make_async_copy(ref, ref, sem).wait()

    def each_inner_row(act):
        for dist in range(rows - 1, 0, -1):
            for step in (dist, -dist):
                target = me_row + step

                @pl.when((target >= 1) & (target <= rows - 2))
                def _():
                    act(target)

    def transform(n):
        g, v0, width = plan[n]
        part = pl.ds(v0, width)
        if g == 0:
            vis_copy(n).wait()
        both = dot(table[g, pl.ds(0, 2 * block), :], vis[0, :, part])
        both = both - dot(table[g, pl.ds(block, 2 * block), :], vis[1, :, part])
        both = both.reshape(2, 2, chips, group, width)
        for ri in range(2):
            pair_out[g, :, pl.ds(ri * group, group), part] = both[ri, 1].astype(BF16)
            mine[g, :, pl.ds(ri * group, group), part] = both[ri, 0]

    def pair_sum(n):
        pair_copy(n).wait_recv()
        g, v0, width = plan[n]
        part = pl.ds(v0, width)
        sums[g, :, :, part] = (mine[g, :, :, part] + pair_in[g, :, :, part].astype(F32)).astype(BF16)

    def col_start(n):
        for target in range(chips):
            @pl.when(target != chip)
            def _():
                col_copy(n, target).start()

    def facet_sum(n):
        g, v0, width = plan[n]
        part = pl.ds(v0, width)
        wait_bytes(others.at[g, pl.ds(0, chips - 1), :, part], col_recv.at[n])
        total = mine[g, chip, :, part] + pair_in[g, chip, :, part].astype(F32)
        for d in range(1, chips):
            total = total + others[g, lax.rem(chip + d, chips), :, part].astype(F32)
        gathered[g, me_row, :, part] = total.astype(BF16)
        each_inner_row(lambda target: row_copy(n, target).start())

    def row_start(at, block_row):
        column0 = (facet_off[1, facet_order[me_col]] + block_row * block_cols) & (NG - 1)
        shape = (m // FINE, block_cols)
        real, imag = cis(iota(shape, 0) * FINE * (column0 + iota(shape, 1)))
        coarse2[at, 0] = real
        coarse2[at, 1] = imag
        shape = (FINE, block_cols)
        real, imag = cis(iota(shape, 0) * (column0 + iota(shape, 1)))
        fine2[at, 0] = real
        fine2[at, 1] = imag
        row_ids = iota((rows, block_cols), 0)
        offsets = jnp.zeros((rows, block_cols), jnp.int32)
        for r in range(rows):
            offsets = jnp.where(row_ids == r, row_off[r], offsets)
        lanes = iota((rows, block_cols), 1)
        beam = 1.0 - BEAM_SLOPE * ((block_row * block_cols + lanes).astype(F32) + 0.5) / FS
        gain = (0.5 / math.sqrt(m * rows)) / beam
        real, imag = cis(offsets * ((column0 + lanes) & (NG - 1)))
        phases[at, 0] = real * gain
        phases[at, 1] = imag * gain

    def row_fill(at, first, last):
        def fill(h, carry):
            a, b = coarse2[at, 0, pl.ds(h, 1), :], coarse2[at, 1, pl.ds(h, 1), :]
            c, d = fine2[at, 0], fine2[at, 1]
            out = pl.ds(pl.multiple_of(h * FINE, FINE), FINE)
            table2[at, 0, out, :] = (a * c - b * d).astype(BF16)
            table2[at, 1, out, :] = (a * d + b * c).astype(BF16)
            return carry

        lax.fori_loop(first, last, fill, 0)

    def second(g, at):
        strongest = best[...]
        for p in range(block_cols // piece):
            part = pl.ds(p * piece, piece)
            sides = []
            for side in range(2):
                v0 = m // 2 if g == GROUPS - 1 else 0
                left = gathered[g, :, :, pl.ds(v0, m - v0)].reshape(rows * 2 * group, m - v0)
                product = dot(left, table2[at, side, pl.ds(v0, m - v0), part])
                if v0:
                    product = product + early[at, side, :, part]
                sides.append(product.reshape(rows, 2, group, piece))
            out_real = jnp.zeros((group, piece), F32)
            out_imag = jnp.zeros((group, piece), F32)
            for r in range(rows):
                real = sides[0][r, 0] - sides[1][r, 1]
                imag = sides[1][r, 0] + sides[0][r, 1]
                a, b = phases[at, 0, pl.ds(r, 1), part], phases[at, 1, pl.ds(r, 1), part]
                out_real = out_real + (real * a - imag * b)
                out_imag = out_imag + (real * b + imag * a)
            if at == 0:
                image[0, 0, pl.ds(g * group, group), part] = out_real
                image[0, 1, pl.ds(g * group, group), part] = out_imag
            else:
                relay_out[g, p, pl.ds(0, group), :] = out_real.astype(BF16)
                relay_out[g, p, pl.ds(group, group), :] = out_imag.astype(BF16)
            power = out_real * out_real + out_imag * out_imag
            power = jnp.max(power.reshape(group // 8, 8, piece), axis=0)
            for lane in range(0, piece, 128):
                strongest = jnp.maximum(strongest, power[:, lane : lane + 128])
        best[...] = strongest
        if at == 1:
            for p in range(block_cols // piece):
                relay_copy(g, p).start()

    def first_half(at):
        left = gathered[GROUPS - 1, :, :, pl.ds(0, m // 2)].reshape(rows * 2 * group, m // 2)
        for side in range(2):
            early[at, side] = dot(left, table2[at, side, pl.ds(0, m // 2), :])

    def when(condition, name, act, *args):
        @pl.when(condition)
        def _():
            with jax.named_scope(name):
                act(*args)

    def arrive(g):
        late = g == GROUPS - 1
        part = pl.ds(m // 2, m // 2) if late else pl.ds(0, m)
        wait_bytes(gathered.at[g, pl.ds(0, rows - 1), :, part], row_recv.at[g + late])

    def arrive_half():
        wait_bytes(gathered.at[GROUPS - 1, pl.ds(0, rows - 1), :, pl.ds(0, m // 2)], row_recv.at[GROUPS - 1])

    def scoped(name, act, *args):
        with jax.named_scope(name):
            act(*args)

    def T(n):
        if plan[n][1] == 0:
            scoped(f"table{n}", column_table, plan[n][0])
        scoped(f"tr{n}", transform, n)
        if n == 0:
            when(inner, "barrier", pl.semaphore_wait, barrier, chips + rows - 1)
            when(outer, "barrier", pl.semaphore_wait, barrier, chips + rows - 2)
        pair_copy(n).start()

    def P(n):
        scoped(f"pair{n}", pair_sum, n)
        when(core == 0, f"col{n}", col_start, n)

    def N(n):
        when(core == 1, f"col{n}", col_start, n)

    def F(n):
        scoped(f"facet{n}", facet_sum, n)

    def R(at):
        when(inner if at == 0 else helps, f"start{at}", row_start, at, me_row if at == 0 else end_row)

    def B(step):
        at, quarter = step // 4, step % 4
        fills = m // FINE // 4
        when(inner if at == 0 else helps, f"fill{step}", row_fill, at, quarter * fills, (quarter + 1) * fills)

    def E(g):
        when(inner, f"arrive{g}", arrive, g)
        when(helps, f"second{g}1", second, g, 1)

    def H(step):
        if step == 0:
            when(inner, "arrivehalf", arrive_half)
            when(helps, "half1", first_half, 1)
        else:
            when(inner, "half0", first_half, 0)

    def S(g):
        when(inner, f"second{g}0", second, g, 0)

    steps = {"T": T, "P": P, "N": N, "F": F, "R": R, "B": B, "E": E, "H": H, "S": S}
    for step in ORDER:
        steps[step[0]](int(step[1:]))

    @pl.when(inner)
    def _():
        peaks[me_row] = jnp.sqrt(best[...])
        for d in range(1, rows):
            peak_copy(peer_row(d)).start()

    @pl.when(outer)
    def _():
        for g in range(GROUPS):
            with jax.named_scope(f"relay{g}"):
                wait_bytes(relay_in.at[g], relay_recv.at[g])
                for p in range(block_cols // piece):
                    for ri in range(2):
                        here = relay_in[g, p, pl.ds(ri * group, group), :]
                        image[0, ri, pl.ds(g * group, group), pl.ds(p * piece, piece)] = here.astype(F32)

    with jax.named_scope("sends"):
        wait_bytes(pair_out, pair_send)
        wait_bytes(others.at[:, pl.ds(0, chips - 1)], col_send)

        @pl.when(outer)
        def _():
            wait_bytes(gathered.at[:, pl.ds(0, rows - 2)], row_send)

        @pl.when(inner)
        def _():
            wait_bytes(gathered.at[:, pl.ds(0, rows - 3)], row_send)

        @pl.when(helps)
        def _():
            wait_bytes(relay_out, relay_send)

    with jax.named_scope("peakwait"):
        @pl.when(outer)
        def _():
            wait_bytes(peaks.at[pl.ds(0, rows - 2)], peak_recv)

        @pl.when(inner)
        def _():
            wait_bytes(peaks.at[pl.ds(0, rows - 3)], peak_recv)
            wait_bytes(peaks.at[pl.ds(0, rows - 1)], peak_send)


def finish_kernel(rows, image, peaks, image_out, peak_out, peak, image_sem, peak_sem):
    copy = pltpu.make_async_copy(image, image_out, image_sem)
    copy.start()
    strongest = peaks[1]
    for r in range(2, rows - 1):
        strongest = jnp.maximum(strongest, peaks[r])
    peak[0] = jnp.max(strongest)
    peak_copy = pltpu.make_async_copy(peak, peak_out, peak_sem)
    peak_copy.start()
    peak_copy.wait()
    copy.wait()


def local(cols, rows, visibilities, col_offsets, row_offsets, facet_offsets, facet_order, vis_counts):
    m = visibilities.shape[1]
    plan = chunk_plan(m)
    chunks = len(plan)
    strips = sum(g == 0 for g, _, _ in plan)
    group = FR // GROUPS
    chips = cols // 2
    block_cols = FS // rows
    piece = min(512, block_cols)

    def blocks(lead, dtype):
        return pltpu.VMEM((GROUPS, lead, 2 * group, m), dtype)

    dma = pltpu.SemaphoreType.DMA
    in_vmem = pl.BlockSpec(memory_space=pltpu.VMEM)
    anywhere = pl.BlockSpec(memory_space=pl.ANY)
    small = (col_offsets, row_offsets, facet_offsets.T, facet_order, vis_counts)
    image, peaks = pl.pallas_call(
        functools.partial(kernel, cols, rows, plan),
        out_shape=(
            pltpu.VMEM((1, 2, FR, block_cols), F32),
            pltpu.VMEM((rows, 8, 128), F32),
        ),
        in_specs=[anywhere] * 6,
        out_specs=(in_vmem, in_vmem),
        scratch_shapes=[pltpu.SMEM(x.shape, x.dtype) for x in small] + [
            dma((len(small),)),
            pltpu.VMEM((2, m, m), BF16),
            pltpu.VMEM((2, cols, m), F32),
            pltpu.VMEM((2, FR, m), F32),
            pltpu.VMEM((GROUPS, 3 * cols * group, m), BF16),
            blocks(chips, F32),
            blocks(chips, BF16),
            blocks(chips, BF16),
            blocks(chips, BF16),
            blocks(chips, BF16),
            blocks(rows, BF16),
            pltpu.VMEM((2, 2, m // FINE, block_cols), F32),
            pltpu.VMEM((2, 2, FINE, block_cols), F32),
            pltpu.VMEM((2, 2, m, block_cols), BF16),
            pltpu.VMEM((2, 2, rows, block_cols), F32),
            pltpu.VMEM((GROUPS, block_cols // piece, 2 * group, piece), BF16),
            pltpu.VMEM((GROUPS, block_cols // piece, 2 * group, piece), BF16),
            pltpu.VMEM((2, 2, rows * 2 * group, block_cols), F32),
            pltpu.VMEM((8, 128), F32),
            dma((strips,)),
            dma,
            dma((chunks,)),
            dma,
            dma((chunks,)),
            dma,
            dma((GROUPS + 1,)),
            dma,
            dma((GROUPS,)),
            dma,
            dma,
        ],
        compiler_params=pltpu.CompilerParams(
            collective_id=0, has_side_effects=True, vmem_limit_bytes=60 * 1024 * 1024),
    )(visibilities, *small)
    return pl.pallas_call(
        functools.partial(finish_kernel, rows),
        out_shape=(jax.ShapeDtypeStruct(image.shape, F32), jax.ShapeDtypeStruct((1,), F32)),
        in_specs=[in_vmem, in_vmem],
        out_specs=(anywhere, anywhere),
        scratch_shapes=[pltpu.SMEM((1,), F32), dma, dma],
        compiler_params=pltpu.CompilerParams(vmem_limit_bytes=1024 * 1024),
    )(image, peaks)


def solution(mesh):
    in_specs = (P(None, "col", "row"), P("col"), P(), P(), P(), P("col", "row"))
    out_specs = (P("col", None, None, "row"), P("col"))
    body = functools.partial(local, mesh.shape["col"], mesh.shape["row"])
    return jax.shard_map(body, mesh=mesh, in_specs=in_specs, out_specs=out_specs, check_vma=False)
```

```python
import functools
import math

import jax
import jax.numpy as jnp
from jax import lax
from jax.experimental import pallas as pl
from jax.experimental.pallas import tpu as pltpu
from jax.sharding import PartitionSpec as P

FS = 4096
NG = 16384
FR = 64
TWO_PI = 2.0 * math.pi
BEAM_SLOPE = 0.66
FINE = 32
GROUPS = 4
ORDER = (
    "T0", "T1", "R0", "P0", "N0", "T2", "P1", "T3", "N1", "P2", "T4", "B0", "B1", "P3", "N2", "T5", "F0", "P4",
    "N3", "T6", "F1", "P5", "N4", "T7", "F2", "P6", "N5", "B2", "B3", "P7", "N6", "N7", "F3", "R1", "B4", "B5",
    "B6", "B7", "F4", "E0", "F5", "S0", "F6", "E1", "F7", "S1", "E2", "S2", "H0", "H1", "E3", "S3",
)
MESH = pl.DeviceIdType.MESH
F32 = jnp.float32
BF16 = jnp.bfloat16


def cis(product):
    shift = (NG // 4).bit_length() - 1
    turn = product & (NG - 1)
    quadrant = (turn + NG // 8) >> shift
    rest = turn - (quadrant << shift)
    angle = rest.astype(F32) * (TWO_PI / NG)
    z = angle * angle
    sine = angle * (1.0 + z * (-1.0 / 6 + z * (1.0 / 120 + z * (-1.0 / 5040 + z * (1.0 / 362880)))))
    cosine = 1.0 + z * (-0.5 + z * (1.0 / 24 + z * (-1.0 / 720 + z * (1.0 / 40320))))
    odd = (quadrant & 1) == 1
    real = jnp.where(odd, sine, cosine)
    imag = jnp.where(odd, cosine, sine)
    real = jnp.where(((quadrant + 1) & 2) != 0, -real, real)
    imag = jnp.where((quadrant & 2) != 0, -imag, imag)
    return real, imag


def iota(shape, dim):
    return lax.broadcasted_iota(jnp.int32, shape, dim)


def chunk_plan(m):
    half = m // 2
    plan = []
    for g in range(GROUPS):
        for h in range(2):
            plan.append((g, h * half, half))
    return plan


def kernel(
    cols, rows, plan,
    vis_hbm, *refs,
):
    small, (image, peaks), scratch = refs[:5], refs[5:7], refs[7:]
    (
    col_off, row_off, facet_off, facet_order, counts, small_sem,
    vis, head, fine, table, mine, pair_out, pair_in, sums, others, gathered,
    coarse2, fine2, table2, phases, relay_out, relay_in, early, best,
    vis_sem, pair_send, pair_recv, col_send, col_recv, row_send, row_recv,
    relay_send, relay_recv, peak_send, peak_recv,
    ) = scratch
    copies = [
        pltpu.make_async_copy(source, target, small_sem.at[n])
        for n, (source, target) in enumerate(zip(small, scratch[:5]))
    ]
    for copy in copies:
        copy.start()
    m = vis.shape[1]
    group = FR // GROUPS
    chips = cols // 2
    block_cols = FS // rows
    piece = min(512, block_cols)
    chunks = len(plan)
    me_col = lax.axis_index("col")
    me_row = lax.axis_index("row")
    core = lax.rem(me_col, 2)
    chip = me_col // 2
    partner = chip * 2 + 1 - core
    inner = (me_row >= 1) & (me_row <= rows - 2)
    outer = (me_row == 0) | (me_row == rows - 1)
    helps = (me_row == 1) | (me_row == rows - 2)
    end_row = jnp.where(me_row <= 1, 0, rows - 1)

    def peer_chip(d):
        return lax.rem(chip + d, chips) * 2 + core

    def peer_row(d):
        return lax.rem(me_row + d, rows)

    barrier = pltpu.get_barrier_semaphore()
    pl.semaphore_signal(barrier, inc=1, device_id=(partner, me_row), device_id_type=MESH)
    for d in range(1, chips):
        pl.semaphore_signal(barrier, inc=1, device_id=(peer_chip(d), me_row), device_id_type=MESH)
    for d in range(1, rows):
        @pl.when(inner | ((peer_row(d) >= 1) & (peer_row(d) <= rows - 2)))
        def _():
            pl.semaphore_signal(barrier, inc=1, device_id=(me_col, peer_row(d)), device_id_type=MESH)

    strips = [(v0, width) for g, v0, width in plan if g == 0]

    def vis_copy(h):
        part = pl.ds(*strips[h])
        return pltpu.make_async_copy(vis_hbm.at[:, :, part], vis.at[:, :, part], vis_sem.at[h])

    for h in range(len(strips)):
        vis_copy(h).start()

    real, imag = cis(iota((FR, m), 0) * iota((FR, m), 1))
    fine[0] = real
    fine[1] = imag
    best[...] = jnp.zeros(best.shape, F32)

    with jax.named_scope("small"):
        for copy in copies:
            copy.wait()

    u = iota((cols, m), 1)
    slot = iota((cols, m), 0)
    start = jnp.zeros((cols, m), jnp.int32)
    for half in range(2):
        for c in range(chips):
            facet = facet_order[c * 2 + (core if half == 0 else 1 - core)]
            first = (facet_off[0, facet] + (FS // 2 - FR // 2)) & (NG - 1)
            start = jnp.where(slot == half * chips + c, first, start)
    real, imag = cis(start * (col_off[0] + u))
    scale = jnp.where(u < counts[0, 0], 1.0 / math.sqrt(m * cols), 0.0)
    head[0] = real * scale
    head[1] = imag * scale
    turns = cis(iota((FR, 128), 0) * col_off[0])
    block = cols * group
    dot = functools.partial(jnp.dot, preferred_element_type=F32)

    def column_table(g):
        rows_here = slice(g * group, (g + 1) * group)
        a, b = (jnp.concatenate([x[rows_here]] * (m // 128), axis=1) for x in turns)
        c, d = fine[0, rows_here, :], fine[1, rows_here, :]
        c, d = a * c - b * d, a * d + b * c
        for s in range(cols):
            a, b = head[0, pl.ds(s, 1), :], head[1, pl.ds(s, 1), :]
            imag = a * d + b * c
            real = a * c - b * d
            table[g, pl.ds(s * group, group), :] = real.astype(BF16)
            table[g, pl.ds(block + s * group, group), :] = imag.astype(BF16)
            table[g, pl.ds(2 * block + s * group, group), :] = (-real).astype(BF16)

    def pair_copy(n):
        g, v0, width = plan[n]
        part = pl.ds(v0, width)
        return pltpu.make_async_remote_copy(
            src_ref=pair_out.at[g, :, :, part], dst_ref=pair_in.at[g, :, :, part],
            send_sem=pair_send, recv_sem=pair_recv.at[n],
            device_id=(partner, me_row), device_id_type=MESH)

    def col_copy(n, target):
        g, v0, width = plan[n]
        part = pl.ds(v0, width)
        return pltpu.make_async_remote_copy(
            src_ref=sums.at[g, target, :, part], dst_ref=others.at[g, chip, :, part],
            send_sem=col_send, recv_sem=col_recv.at[n],
            device_id=(target * 2 + core, me_row), device_id_type=MESH)

    def row_copy(n, target):
        g, v0, width = plan[n]
        part = pl.ds(v0, width)
        return pltpu.make_async_remote_copy(
            src_ref=gathered.at[g, me_row, :, part], dst_ref=gathered.at[g, me_row, :, part],
            send_sem=row_send, recv_sem=row_recv.at[g + (g == GROUPS - 1 and v0 >= m // 2)],
            device_id=(me_col, target), device_id_type=MESH)

    def relay_copy(g, p):
        return pltpu.make_async_remote_copy(
            src_ref=relay_out.at[g, p], dst_ref=relay_in.at[g, p],
            send_sem=relay_send, recv_sem=relay_recv.at[g],
            device_id=(me_col, end_row), device_id_type=MESH)

    def peak_copy(target):
        return pltpu.make_async_remote_copy(
            src_ref=peaks.at[me_row], dst_ref=peaks.at[me_row],
            send_sem=peak_send, recv_sem=peak_recv,
            device_id=(me_col, target), device_id_type=MESH)

    def wait_bytes(ref, sem):
        pltpu.make_async_copy(ref, ref, sem).wait()

    def each_inner_row(act):
        for dist in range(rows - 1, 0, -1):
            for step in (dist, -dist):
                target = me_row + step

                @pl.when((target >= 1) & (target <= rows - 2))
                def _():
                    act(target)

    def transform(n):
        g, v0, width = plan[n]
        part = pl.ds(v0, width)
        if g == 0:
            vis_copy(n).wait()
        both = dot(table[g, pl.ds(0, 2 * block), :], vis[0, :, part])
        both = both - dot(table[g, pl.ds(block, 2 * block), :], vis[1, :, part])
        both = both.reshape(2, 2, chips, group, width)
        for ri in range(2):
            pair_out[g, :, pl.ds(ri * group, group), part] = both[ri, 1].astype(BF16)
            mine[g, :, pl.ds(ri * group, group), part] = both[ri, 0]

    def pair_sum(n):
        pair_copy(n).wait_recv()
        g, v0, width = plan[n]
        part = pl.ds(v0, width)
        sums[g, :, :, part] = (mine[g, :, :, part] + pair_in[g, :, :, part].astype(F32)).astype(BF16)

    def col_start(n):
        for target in range(chips):
            @pl.when(target != chip)
            def _():
                col_copy(n, target).start()

    def facet_sum(n):
        g, v0, width = plan[n]
        part = pl.ds(v0, width)
        wait_bytes(others.at[g, pl.ds(0, chips - 1), :, part], col_recv.at[n])
        total = mine[g, chip, :, part] + pair_in[g, chip, :, part].astype(F32)
        for d in range(1, chips):
            total = total + others[g, lax.rem(chip + d, chips), :, part].astype(F32)
        gathered[g, me_row, :, part] = total.astype(BF16)
        each_inner_row(lambda target: row_copy(n, target).start())

    def row_start(at, block_row):
        column0 = (facet_off[1, facet_order[me_col]] + block_row * block_cols) & (NG - 1)
        shape = (m // FINE, block_cols)
        real, imag = cis(iota(shape, 0) * FINE * (column0 + iota(shape, 1)))
        coarse2[at, 0] = real
        coarse2[at, 1] = imag
        shape = (FINE, block_cols)
        real, imag = cis(iota(shape, 0) * (column0 + iota(shape, 1)))
        fine2[at, 0] = real
        fine2[at, 1] = imag
        row_ids = iota((rows, block_cols), 0)
        offsets = jnp.zeros((rows, block_cols), jnp.int32)
        for r in range(rows):
            offsets = jnp.where(row_ids == r, row_off[r], offsets)
        lanes = iota((rows, block_cols), 1)
        beam = 1.0 - BEAM_SLOPE * ((block_row * block_cols + lanes).astype(F32) + 0.5) / FS
        gain = (0.5 / math.sqrt(m * rows)) / beam
        real, imag = cis(offsets * ((column0 + lanes) & (NG - 1)))
        phases[at, 0] = real * gain
        phases[at, 1] = imag * gain

    def row_fill(at, first, last):
        def fill(h, carry):
            a, b = coarse2[at, 0, pl.ds(h, 1), :], coarse2[at, 1, pl.ds(h, 1), :]
            c, d = fine2[at, 0], fine2[at, 1]
            out = pl.ds(pl.multiple_of(h * FINE, FINE), FINE)
            table2[at, 0, out, :] = (a * c - b * d).astype(BF16)
            table2[at, 1, out, :] = (a * d + b * c).astype(BF16)
            return carry

        lax.fori_loop(first, last, fill, 0)

    def second(g, at):
        strongest = best[...]
        for p in range(block_cols // piece):
            part = pl.ds(p * piece, piece)
            sides = []
            for side in range(2):
                v0 = m // 2 if g == GROUPS - 1 else 0
                left = gathered[g, :, :, pl.ds(v0, m - v0)].reshape(rows * 2 * group, m - v0)
                product = dot(left, table2[at, side, pl.ds(v0, m - v0), part])
                if v0:
                    product = product + early[at, side, :, part]
                sides.append(product.reshape(rows, 2, group, piece))
            out_real = jnp.zeros((group, piece), F32)
            out_imag = jnp.zeros((group, piece), F32)
            for r in range(rows):
                real = sides[0][r, 0] - sides[1][r, 1]
                imag = sides[1][r, 0] + sides[0][r, 1]
                a, b = phases[at, 0, pl.ds(r, 1), part], phases[at, 1, pl.ds(r, 1), part]
                out_real = out_real + (real * a - imag * b)
                out_imag = out_imag + (real * b + imag * a)
            if at == 0:
                image[0, 0, pl.ds(g * group, group), part] = out_real
                image[0, 1, pl.ds(g * group, group), part] = out_imag
            else:
                relay_out[g, p, pl.ds(0, group), :] = out_real.astype(BF16)
                relay_out[g, p, pl.ds(group, group), :] = out_imag.astype(BF16)
            power = out_real * out_real + out_imag * out_imag
            power = jnp.max(power.reshape(group // 8, 8, piece), axis=0)
            for lane in range(0, piece, 128):
                strongest = jnp.maximum(strongest, power[:, lane : lane + 128])
        best[...] = strongest
        if at == 1:
            for p in range(block_cols // piece):
                relay_copy(g, p).start()

    def first_half(at):
        left = gathered[GROUPS - 1, :, :, pl.ds(0, m // 2)].reshape(rows * 2 * group, m // 2)
        for side in range(2):
            early[at, side] = dot(left, table2[at, side, pl.ds(0, m // 2), :])

    def when(condition, name, act, *args):
        @pl.when(condition)
        def _():
            with jax.named_scope(name):
                act(*args)

    def arrive(g):
        late = g == GROUPS - 1
        part = pl.ds(m // 2, m // 2) if late else pl.ds(0, m)
        wait_bytes(gathered.at[g, pl.ds(0, rows - 1), :, part], row_recv.at[g + late])

    def arrive_half():
        wait_bytes(gathered.at[GROUPS - 1, pl.ds(0, rows - 1), :, pl.ds(0, m // 2)], row_recv.at[GROUPS - 1])

    def scoped(name, act, *args):
        with jax.named_scope(name):
            act(*args)

    def T(n):
        if plan[n][1] == 0:
            scoped(f"table{n}", column_table, plan[n][0])
        scoped(f"tr{n}", transform, n)
        if n == 0:
            when(inner, "barrier", pl.semaphore_wait, barrier, chips + rows - 1)
            when(outer, "barrier", pl.semaphore_wait, barrier, chips + rows - 2)
        pair_copy(n).start()

    def P(n):
        scoped(f"pair{n}", pair_sum, n)
        when(core == 0, f"col{n}", col_start, n)

    def N(n):
        when(core == 1, f"col{n}", col_start, n)

    def F(n):
        scoped(f"facet{n}", facet_sum, n)

    def R(at):
        when(inner if at == 0 else helps, f"start{at}", row_start, at, me_row if at == 0 else end_row)

    def B(step):
        at, quarter = step // 4, step % 4
        fills = m // FINE // 4
        when(inner if at == 0 else helps, f"fill{step}", row_fill, at, quarter * fills, (quarter + 1) * fills)

    def E(g):
        when(inner, f"arrive{g}", arrive, g)
        when(helps, f"second{g}1", second, g, 1)

    def H(step):
        if step == 0:
            when(inner, "arrivehalf", arrive_half)
            when(helps, "half1", first_half, 1)
        else:
            when(inner, "half0", first_half, 0)

    def S(g):
        when(inner, f"second{g}0", second, g, 0)

    steps = {"T": T, "P": P, "N": N, "F": F, "R": R, "B": B, "E": E, "H": H, "S": S}
    for step in ORDER:
        steps[step[0]](int(step[1:]))

    @pl.when(inner)
    def _():
        peaks[me_row] = jnp.sqrt(best[...])
        for d in range(1, rows):
            peak_copy(peer_row(d)).start()

    @pl.when(outer)
    def _():
        for g in range(GROUPS):
            with jax.named_scope(f"relay{g}"):
                wait_bytes(relay_in.at[g], relay_recv.at[g])
                for p in range(block_cols // piece):
                    for ri in range(2):
                        here = relay_in[g, p, pl.ds(ri * group, group), :]
                        image[0, ri, pl.ds(g * group, group), pl.ds(p * piece, piece)] = here.astype(F32)

    with jax.named_scope("sends"):
        wait_bytes(pair_out, pair_send)
        wait_bytes(others.at[:, pl.ds(0, chips - 1)], col_send)

        @pl.when(outer)
        def _():
            wait_bytes(gathered.at[:, pl.ds(0, rows - 2)], row_send)

        @pl.when(inner)
        def _():
            wait_bytes(gathered.at[:, pl.ds(0, rows - 3)], row_send)

        @pl.when(helps)
        def _():
            wait_bytes(relay_out, relay_send)

    with jax.named_scope("peakwait"):
        @pl.when(outer)
        def _():
            wait_bytes(peaks.at[pl.ds(0, rows - 2)], peak_recv)

        @pl.when(inner)
        def _():
            wait_bytes(peaks.at[pl.ds(0, rows - 3)], peak_recv)
            wait_bytes(peaks.at[pl.ds(0, rows - 1)], peak_send)


def finish_kernel(rows, image, peaks, image_out, peak_out, peak, image_sem, peak_sem):
    copy = pltpu.make_async_copy(image, image_out, image_sem)
    copy.start()
    strongest = peaks[1]
    for r in range(2, rows - 1):
        strongest = jnp.maximum(strongest, peaks[r])
    peak[0] = jnp.max(strongest)
    peak_copy = pltpu.make_async_copy(peak, peak_out, peak_sem)
    peak_copy.start()
    peak_copy.wait()
    copy.wait()


def local(cols, rows, visibilities, col_offsets, row_offsets, facet_offsets, facet_order, vis_counts):
    m = visibilities.shape[1]
    plan = chunk_plan(m)
    chunks = len(plan)
    strips = sum(g == 0 for g, _, _ in plan)
    group = FR // GROUPS
    chips = cols // 2
    block_cols = FS // rows
    piece = min(512, block_cols)

    def blocks(lead, dtype):
        return pltpu.VMEM((GROUPS, lead, 2 * group, m), dtype)

    dma = pltpu.SemaphoreType.DMA
    in_vmem = pl.BlockSpec(memory_space=pltpu.VMEM)
    anywhere = pl.BlockSpec(memory_space=pl.ANY)
    small = (col_offsets, row_offsets, facet_offsets.T, facet_order, vis_counts)
    image, peaks = pl.pallas_call(
        functools.partial(kernel, cols, rows, plan),
        out_shape=(
            pltpu.VMEM((1, 2, FR, block_cols), F32),
            pltpu.VMEM((rows, 8, 128), F32),
        ),
        in_specs=[anywhere] * 6,
        out_specs=(in_vmem, in_vmem),
        scratch_shapes=[pltpu.SMEM(x.shape, x.dtype) for x in small] + [
            dma((len(small),)),
            pltpu.VMEM((2, m, m), BF16),
            pltpu.VMEM((2, cols, m), F32),
            pltpu.VMEM((2, FR, m), F32),
            pltpu.VMEM((GROUPS, 3 * cols * group, m), BF16),
            blocks(chips, F32),
            blocks(chips, BF16),
            blocks(chips, BF16),
            blocks(chips, BF16),
            blocks(chips, BF16),
            blocks(rows, BF16),
            pltpu.VMEM((2, 2, m // FINE, block_cols), F32),
            pltpu.VMEM((2, 2, FINE, block_cols), F32),
            pltpu.VMEM((2, 2, m, block_cols), BF16),
            pltpu.VMEM((2, 2, rows, block_cols), F32),
            pltpu.VMEM((GROUPS, block_cols // piece, 2 * group, piece), BF16),
            pltpu.VMEM((GROUPS, block_cols // piece, 2 * group, piece), BF16),
            pltpu.VMEM((2, 2, rows * 2 * group, block_cols), F32),
            pltpu.VMEM((8, 128), F32),
            dma((strips,)),
            dma,
            dma((chunks,)),
            dma,
            dma((chunks,)),
            dma,
            dma((GROUPS + 1,)),
            dma,
            dma((GROUPS,)),
            dma,
            dma,
        ],
        compiler_params=pltpu.CompilerParams(
            collective_id=0, has_side_effects=True, vmem_limit_bytes=60 * 1024 * 1024),
    )(visibilities, *small)
    return pl.pallas_call(
        functools.partial(finish_kernel, rows),
        out_shape=(jax.ShapeDtypeStruct(image.shape, F32), jax.ShapeDtypeStruct((1,), F32)),
        in_specs=[in_vmem, in_vmem],
        out_specs=(anywhere, anywhere),
        scratch_shapes=[pltpu.SMEM((1,), F32), dma, dma],
        compiler_params=pltpu.CompilerParams(vmem_limit_bytes=1024 * 1024),
    )(image, peaks)


def solution(mesh):
    in_specs = (P(None, "col", "row"), P("col"), P(), P(), P(), P("col", "row"))
    out_specs = (P("col", None, None, "row"), P("col"))
    body = functools.partial(local, mesh.shape["col"], mesh.shape["row"])
    return jax.shard_map(body, mesh=mesh, in_specs=in_specs, out_specs=out_specs, check_vma=False)
```
